128 devices in a mesh: grid: 8 (over z, core), dom: 16 (over y, x).
Axes of the slice: x: 4, y: 4, z: 4, core: 2. Of those that a mesh axis runs over, the one named last changes fastest.
Arguments:
- columns: bfloat16 [262144, 128], P(('grid', 'dom')), may hold values from -6 to 6
- column_live: int32 [262144], P(('grid', 'dom')), may hold values 0 or 1
- col_weight: float32 [262144], P(('grid', 'dom')), may hold values from 0.2 to 1
- col_slot: int32 [262144], P(('grid', 'dom')), may hold values from 0 to 511
- node_static: bfloat16 [65536, 256], P(('grid', 'dom')), may hold values from -6 to 6
- boundary_idx: int32 [32768], P(('grid', 'dom')), may hold values from 0 to 511
- edge_src: int32 [262144], P(('grid', 'dom')), may hold values from 0 to 1535
- edge_dst: int32 [262144], P(('grid', 'dom')), may hold values from 0 to 511
- edge_live: int32 [262144], P(('grid', 'dom')), may hold values from 0 to 1, as said below
- edge_weight: float32 [262144], P(('grid', 'dom')), may hold values from 0.2 to 1
- enc_in: bfloat16 [128, 256], replicated, may hold values from -0.5 to 0.5
- enc_out: bfloat16 [256, 256], replicated, may hold values from -0.375 to 0.375
- src_proj: bfloat16 [2, 256, 256], replicated, may hold values from -0.375 to 0.375
- dst_proj: bfloat16 [2, 256, 256], replicated, may hold values from -0.375 to 0.375
- msg_proj: bfloat16 [2, 256, 256], replicated, may hold values from -0.375 to 0.375
- node_cotangent: bfloat16 [65536, 256], P(('grid', 'dom')), may hold values from -6 to 6
Outputs:
- node_out: bfloat16 [65536, 256], P(('grid', 'dom'))
- enc_in_grad: float32 [128, 256], replicated
- enc_out_grad: float32 [256, 256], replicated
- src_grad: float32 [2, 256, 256], replicated
- dst_grad: float32 [2, 256, 256], replicated
- msg_grad: float32 [2, 256, 256], replicated
The draws below stay inside these ranges and needn't reach their ends.
Inputs may be any that keep to these rules, and one draw needn't show every extreme that they name: `col_slot`: column slot j of a partition, with k * 16 <= j < (k + 1) * 16, is bound for partition k. `edge_src`: values below 512 are the partition's own nodes; 512 + r * 256 + i is boundary entry i of neighbour r (r = 0 to 3 as in the reference program). `edge_live`: in each partition the live edge slots come first; some partition has all 2048 live.
All inputs are finite; a program needn't handle non-finite values. No bound on the sum of `column_live` on one device may be relied on, other than what follows from the above.
Results may differ from the reference program's by a relative error of at most 0.0095.
Values may be sent and summed in bfloat16 or wider, within the bound.
A program may use at most 128 MiB of HBM per device.

```python
import jax
import jax.numpy as jnp
from jax import lax

H = 256
FIN = 128
LAYERS = 2
NODE_DEV = 512
E_DEV = 2048
BND = 256
COL_DEV = 2048
NODES = 65536
EDGES = 262144
BOUNDS = 32768
COLUMNS = 262144
EXT = 1536
N_GRID = 8
N_DOM = 16
DEVICES = 128


def draw_edge_live(key, part):
    first_key, second_key = jax.random.split(jax.random.fold_in(key, 11))
    raw_counts = jax.random.randint(first_key, (DEVICES,), 0, E_DEV + 1)
    counts = jnp.maximum(raw_counts * raw_counts // E_DEV, E_DEV // 16)
    fullest = jax.random.randint(second_key, (), 0, DEVICES)
    counts = jnp.where(jnp.arange(DEVICES) == fullest, E_DEV, counts)
    positions = jnp.arange(E_DEV)
    return (positions[None, :] < counts[:, None]).astype(jnp.int32).reshape(DEVICES * E_DEV)


def set_ends(result, own_key, low, top_value):
    extent = result.shape
    index_at = [jax.random.randint(jax.random.fold_in(own_key, axis), (), 0, extent[axis]) for axis in range(len(extent))]
    result = result.at[tuple(index_at)].set(low)
    longest = extent.index(max(extent))
    index_at[longest] = (index_at[longest] + 1) % extent[longest]
    return result.at[tuple(index_at)].set(top_value)


def levels(stream_key, dims, cuts, smallest, largest):
    def one(dim, blocks):
        heights = jax.random.uniform(jax.random.fold_in(jax.random.fold_in(stream_key, 6), dim), (blocks,), jnp.float32, smallest / len(cuts), largest / len(cuts))
        return jnp.repeat(jnp.exp(heights), dims[dim] // blocks).reshape((-1,) + (1,) * (len(dims) - dim - 1))

    loudness = one(*cuts[0])
    for cut in cuts[1:]:
        loudness = loudness * one(*cut)
    return loudness


def bell_draw(stream_key, dims, spread, bound, cuts=(), held_as=jnp.bfloat16):
    level = levels(stream_key, dims, cuts, -0.22, 0.18) if cuts else 1.0
    entries = jax.random.normal(stream_key, dims, jnp.float32) * spread * level
    return jnp.minimum(jnp.maximum(entries, -bound), bound).astype(held_as)


def setup_inputs(seed: int = 0) -> dict:
    arg_keys = jax.random.split(jax.random.key(seed), 17)
    return {
        "columns": bell_draw(arg_keys[0], (COLUMNS, FIN), 1.0, 6.0, ((0, 128),)),
        "column_live": set_ends((jax.random.randint(arg_keys[1], (COLUMNS,), 0, 2) < 1).astype(jnp.int32), jax.random.fold_in(arg_keys[1], 1), 0, 1),
        "col_weight": jnp.clip(0.2 + 0.8 * jax.random.uniform(arg_keys[2], (COLUMNS,), jnp.float32) ** levels(arg_keys[2], (COLUMNS,), ((0, 128),), -0.2, 0.2), 0.2, 1.0),
        "col_slot": set_ends(jax.random.randint(arg_keys[3], (COLUMNS,), 0, NODE_DEV), jax.random.fold_in(arg_keys[3], 1), 0, NODE_DEV - 1).astype(jnp.int32),
        "node_static": bell_draw(arg_keys[4], (NODES, H), 1.0, 6.0, ((0, 128),)),
        "boundary_idx": set_ends(jax.random.randint(arg_keys[5], (BOUNDS,), 0, NODE_DEV), jax.random.fold_in(arg_keys[5], 1), 0, NODE_DEV - 1).astype(jnp.int32),
        "edge_src": set_ends(jax.random.randint(arg_keys[6], (EDGES,), 0, EXT), jax.random.fold_in(arg_keys[6], 1), 0, EXT - 1).astype(jnp.int32),
        "edge_dst": set_ends(jax.random.randint(arg_keys[7], (EDGES,), 0, NODE_DEV), jax.random.fold_in(arg_keys[7], 1), 0, NODE_DEV - 1).astype(jnp.int32),
        "edge_live": draw_edge_live(jax.random.fold_in(arg_keys[16], 71), 0),
        "edge_weight": jnp.clip(0.2 + 0.8 * jax.random.uniform(arg_keys[9], (EDGES,), jnp.float32) ** levels(arg_keys[9], (EDGES,), ((0, 128),), -0.2, 0.2), 0.2, 1.0),
        "enc_in": bell_draw(arg_keys[10], (FIN, H), FIN ** -0.5, 0.5),
        "enc_out": bell_draw(arg_keys[11], (H, H), H ** -0.5, 0.375),
        "src_proj": bell_draw(arg_keys[12], (LAYERS, H, H), H ** -0.5, 0.375),
        "dst_proj": bell_draw(arg_keys[13], (LAYERS, H, H), H ** -0.5, 0.375),
        "msg_proj": bell_draw(arg_keys[14], (LAYERS, H, H), H ** -0.5, 0.375),
        "node_cotangent": bell_draw(arg_keys[15], (NODES, H), 1.0, 6.0, ((0, 128),)),
    }


def silu_grad(inputs):
    sigmoid_val = jax.nn.sigmoid(inputs)
    return sigmoid_val * (1.0 + inputs * (1.0 - sigmoid_val))

def outer_sum(left_side, right_side):
    return lax.dot_general(left_side, right_side, (((0,), (0,)), ((), ())), preferred_element_type=jnp.float32)

def times_transpose(left_side, right_side):
    return lax.dot_general(left_side, right_side, (((1,), (1,)), ((), ())), preferred_element_type=jnp.float32)

def pick_rows(rows_all, indices):
    return rows_all[indices]

def scatter_rows(values, indices):
    return jax.ops.segment_sum(values, indices, num_segments=NODE_DEV)

def grid_view(blocks):
    return blocks.reshape((N_GRID, N_DOM) + blocks.shape[1:])

def shifted(blocks, axis_pos, offset):
    length = blocks.shape[axis_pos]
    blank_row = jnp.zeros_like(lax.slice_in_dim(blocks, 0, 1, axis=axis_pos))
    if offset > 0:
        return jnp.concatenate([blank_row, lax.slice_in_dim(blocks, 0, length - 1, axis=axis_pos)], axis_pos)
    return jnp.concatenate([lax.slice_in_dim(blocks, 1, length, axis=axis_pos), blank_row], axis_pos)

def neighbour_rims(node_state, rim_idx):
    rims = grid_view(jax.vmap(pick_rows)(node_state, rim_idx))
    stacked = jnp.stack([shifted(rims, 0, 1), shifted(rims, 0, -1), shifted(rims, 1, 1), shifted(rims, 1, -1)], 2)
    return stacked.reshape(DEVICES, 4 * BND, H)

def reference(columns, column_live, col_weight, col_slot, node_static, boundary_idx, edge_src, edge_dst, edge_live, edge_weight, enc_in, enc_out, src_proj, dst_proj, msg_proj, node_cotangent):
    bucket = COL_DEV // DEVICES
    col_blocks = columns.reshape(DEVICES, COL_DEV, FIN)
    scale_blocks = (col_weight * column_live.astype(jnp.float32)).reshape(DEVICES, COL_DEV)
    edge_scale = (edge_weight * edge_live.astype(jnp.float32)).reshape(DEVICES, E_DEV)
    src_blocks = edge_src.reshape(DEVICES, E_DEV)
    dst_blocks = edge_dst.reshape(DEVICES, E_DEV)
    rim_idx = boundary_idx.reshape(DEVICES, BND)

    def encode_one(pieces):
        col_rows, col_scale = pieces
        enc_pre = jnp.dot(col_rows, enc_in, preferred_element_type=jnp.float32)
        enc_act = jax.nn.silu(enc_pre).astype(jnp.bfloat16)
        return (jnp.dot(enc_act, enc_out, preferred_element_type=jnp.float32) * col_scale[:, None]).astype(jnp.bfloat16)
    col_embed = lax.map(encode_one, (col_blocks, scale_blocks))
    arrived = col_embed.reshape(DEVICES, DEVICES, bucket, H).transpose(1, 0, 2, 3).reshape(DEVICES, COL_DEV, H)
    arrived_slots = col_slot.reshape(DEVICES, DEVICES, bucket).transpose(1, 0, 2).reshape(DEVICES, COL_DEV)

    def pool_one(pieces):
        rows_in, slots_in, static_rows = pieces
        pooled = jax.ops.segment_sum(rows_in.astype(jnp.float32), slots_in, num_segments=NODE_DEV)
        return (static_rows.astype(jnp.float32) + pooled).astype(jnp.bfloat16)
    node_state = lax.map(pool_one, (arrived, arrived_slots, node_static.reshape(DEVICES, NODE_DEV, H)))
    states = []
    for layer_idx in range(LAYERS):
        src_w = src_proj[layer_idx]
        dst_w = dst_proj[layer_idx]
        msg_w = msg_proj[layer_idx]

        def forward_one(pieces):
            own_rows, rim_rows, src_idx, dst_idx, scale_row = pieces
            src_table = jnp.concatenate([own_rows, rim_rows], 0)
            from_src = jnp.dot(src_table, src_w, preferred_element_type=jnp.float32)
            from_dst = jnp.dot(own_rows, dst_w, preferred_element_type=jnp.float32)
            pre_edge = from_src[src_idx] + from_dst[dst_idx]
            act_edge = jax.nn.silu(pre_edge).astype(jnp.bfloat16)
            message = jnp.dot(act_edge, msg_w, preferred_element_type=jnp.float32) * scale_row[:, None]
            gathered = jax.ops.segment_sum(message, dst_idx, num_segments=NODE_DEV)
            return (own_rows.astype(jnp.float32) + gathered).astype(jnp.bfloat16)
        states.append(node_state)
        rims_now = neighbour_rims(node_state, rim_idx)
        node_state = lax.map(forward_one, (node_state, rims_now, src_blocks, dst_blocks, edge_scale))
    node_out = node_state.reshape(NODES, H)
    grad_state = node_cotangent.astype(jnp.float32).reshape(DEVICES, NODE_DEV, H)
    src_terms = [None] * LAYERS
    dst_terms = [None] * LAYERS
    msg_terms = [None] * LAYERS
    for layer_idx in reversed(range(LAYERS)):
        src_w = src_proj[layer_idx]
        dst_w = dst_proj[layer_idx]
        msg_w = msg_proj[layer_idx]

        def backward_one(pieces):
            own_rows, rim_rows, src_idx, dst_idx, scale_row, grad_out = pieces
            src_table = jnp.concatenate([own_rows, rim_rows], 0)
            from_src = jnp.dot(src_table, src_w, preferred_element_type=jnp.float32)
            from_dst = jnp.dot(own_rows, dst_w, preferred_element_type=jnp.float32)
            pre_edge = from_src[src_idx] + from_dst[dst_idx]
            act_edge = jax.nn.silu(pre_edge).astype(jnp.bfloat16)
            grad_msg = (grad_out[dst_idx] * scale_row[:, None]).astype(jnp.bfloat16)
            msg_term = outer_sum(act_edge, grad_msg)
            grad_act = times_transpose(grad_msg, msg_w)
            grad_pre = grad_act * silu_grad(pre_edge)
            grad_src = jax.ops.segment_sum(grad_pre, src_idx, num_segments=NODE_DEV + 4 * BND).astype(jnp.bfloat16)
            grad_dst = jax.ops.segment_sum(grad_pre, dst_idx, num_segments=NODE_DEV).astype(jnp.bfloat16)
            src_term = outer_sum(src_table, grad_src)
            dst_term = outer_sum(own_rows, grad_dst)
            grad_table = times_transpose(grad_src, src_w)
            grad_own = grad_out + grad_table[:NODE_DEV] + times_transpose(grad_dst, dst_w)
            return (grad_own, grad_table[NODE_DEV:].reshape(4, BND, H), src_term, dst_term, msg_term)
        own_state = states[layer_idx]
        rims_now = neighbour_rims(own_state, rim_idx)
        grad_own, grad_rims, src_all, dst_all, msg_all = lax.map(backward_one, (own_state, rims_now, src_blocks, dst_blocks, edge_scale, grad_state))
        src_terms[layer_idx] = lax.optimization_barrier(jnp.sum(src_all, 0))
        dst_terms[layer_idx] = lax.optimization_barrier(jnp.sum(dst_all, 0))
        msg_terms[layer_idx] = lax.optimization_barrier(jnp.sum(msg_all, 0))
        returned = grid_view(grad_rims)
        rim_grad = shifted(returned[:, :, 0], 0, -1) + shifted(returned[:, :, 1], 0, 1) + shifted(returned[:, :, 2], 1, -1) + shifted(returned[:, :, 3], 1, 1)
        grad_state = grad_own + jax.vmap(scatter_rows)(rim_grad.reshape(DEVICES, BND, H), rim_idx)
    grad_nodes = grad_state.astype(jnp.bfloat16)
    back_rows = jax.vmap(pick_rows)(grad_nodes, arrived_slots)
    grad_embed = back_rows.reshape(DEVICES, DEVICES, bucket, H).transpose(1, 0, 2, 3).reshape(DEVICES, COL_DEV, H)

    def encode_back(pieces):
        col_rows, col_scale, grad_rows = pieces
        enc_pre = jnp.dot(col_rows, enc_in, preferred_element_type=jnp.float32)
        enc_act = jax.nn.silu(enc_pre).astype(jnp.bfloat16)
        grad_enc = (grad_rows.astype(jnp.float32) * col_scale[:, None]).astype(jnp.bfloat16)
        out_term = outer_sum(enc_act, grad_enc)
        grad_act = times_transpose(grad_enc, enc_out)
        grad_pre = (grad_act * silu_grad(enc_pre)).astype(jnp.bfloat16)
        in_term = outer_sum(col_rows, grad_pre)
        return (in_term, out_term)
    in_all, out_all = lax.map(encode_back, (col_blocks, scale_blocks, grad_embed))
    enc_in_grad = lax.optimization_barrier(jnp.sum(in_all, 0))
    enc_out_grad = lax.optimization_barrier(jnp.sum(out_all, 0))
    return (node_out, enc_in_grad, enc_out_grad, jnp.stack(src_terms, 0), jnp.stack(dst_terms, 0), jnp.stack(msg_terms, 0))
```

```python
import functools

import jax
import jax.numpy as jnp
from jax import lax
from jax.experimental import pallas as pl
from jax.experimental.pallas import tpu as pltpu
from jax.sharding import PartitionSpec as P

MESH = pl.DeviceIdType.MESH
BF = jnp.bfloat16
F32 = jnp.float32
CH = 256
LANES = 128
TILE = 16


def mm(a, b):
    return lax.dot_general(a, b, (((1,), (0,)), ((), ())), preferred_element_type=F32)


def mt(a, b):
    return lax.dot_general(a, b, (((1,), (1,)), ((), ())), preferred_element_type=F32)


def tm(a, b):
    return lax.dot_general(a, b, (((0,), (0,)), ((), ())), preferred_element_type=F32)


def wide(x):
    return jnp.concatenate([x, x], axis=1)


def hot(equal):
    return jnp.where(equal, 1.0, 0.0).astype(BF)


def step_kernel(
    n_grid, n_dom,
    cols, live, cweight, slot, static, bidx, esrc, edst, elive, eweight,
    enc_in, enc_out, src_proj, dst_proj, msg_proj, cot,
    node_out, gall,
    aux_tx, aux_rx, rx, srow, crow, ccol, ecol,
    so, sr, sot, srt, dd, ddt, bb, bbt, pp, ppt,
    hh, rim, rim_tx, gt_tx, gt_rx,
    eact, edsilu, cemb, pre0, pre1, act0, act1, msg, gm0, gm1, ga1, gp, gs_own, gs_rim, gd, gh,
    acc, g1, g0, ge, gr, ag,
    a2a_send, a2a_recv, aux_send, aux_recv, rim_send, rim_recv, gt_send, gt_recv,
    rs_send, rs_recv, ag_send, ag_recv, own_sem,
):
    n_dev = n_grid * n_dom
    n_node = static.shape[0]
    n_edge = so.shape[0]
    n_col = cols.shape[0]
    n_bnd = bb.shape[0]
    rows_e = n_edge // LANES
    rows_c = n_col // LANES
    g = lax.axis_index("grid")
    o = lax.axis_index("dom")
    me = g * n_dom + o

    def coords(d):
        return (d // n_dom, lax.rem(d, n_dom))

    def others(fn):
        def body(k, carry):
            fn(lax.rem(me + k, n_dev))
            return carry
        lax.fori_loop(1, n_dev, body, 0)

    def loop(n, fn):
        def body(k, carry):
            fn(k)
            return carry
        lax.fori_loop(0, n, body, 0)

    barrier = pltpu.get_barrier_semaphore()
    others(lambda d: pl.semaphore_signal(barrier, inc=1, device_id=coords(d), device_id_type=MESH))

    lane = lax.broadcasted_iota(jnp.int32, (rows_c, LANES), 1)
    quarter = lax.rem(me, 4)
    slot_f = slot[...].astype(F32)
    scale_f = cweight[...] * live[...].astype(F32)
    for j in range(8):
        to_slot = lax.rem((quarter - j) * 16 + 2 * LANES, LANES)
        to_scale = lax.rem((quarter - j) * 16 + 64 + 2 * LANES, LANES)
        a = pltpu.roll(slot_f, to_slot, axis=1)
        b = pltpu.roll(scale_f, to_scale, axis=1)
        row = jnp.where(lane // 16 == quarter, a, jnp.where(lane // 16 == quarter + 4, b, 0.0))
        aux_tx[pl.ds(j, rows_c, stride=8), :] = row

    pl.semaphore_wait(barrier, n_dev - 1)

    def send_cols(d):
        pltpu.make_async_remote_copy(
            src_ref=cols.at[pl.ds(pl.multiple_of(d * TILE, TILE), TILE), :],
            dst_ref=rx.at[pl.ds(pl.multiple_of(me * TILE, TILE), TILE), :],
            send_sem=a2a_send, recv_sem=a2a_recv, device_id=coords(d), device_id_type=MESH,
        ).start()
        pltpu.make_async_remote_copy(
            src_ref=aux_tx.at[d], dst_ref=aux_rx.at[me],
            send_sem=aux_send, recv_sem=aux_recv, device_id=coords(d), device_id_type=MESH,
        ).start()

    others(send_cols)
    mine = pl.ds(pl.multiple_of(me * TILE, TILE), TILE)
    rx[mine, :] = cols[mine, :]
    aux_rx[me] = aux_tx[me]

    here = (g > 0, g < n_grid - 1, o > 0, o < n_dom - 1)
    near = ((g - 1, o), (g + 1, o), (g, o - 1), (g, o + 1))
    flip = (1, 0, 3, 2)
    for r in range(4):
        @pl.when(jnp.logical_not(here[r]))
        def _():
            for l in range(2):
                rim[l, r] = jnp.zeros((n_bnd, 256), BF)
                gt_rx[l, flip[r]] = jnp.zeros((n_bnd, 256), BF)

    lane_i = lax.broadcasted_iota(jnp.int32, (LANES, LANES), 1)
    sub_i = lax.broadcasted_iota(jnp.int32, (LANES, LANES), 0)

    def across(row):
        full = jnp.broadcast_to(row, (LANES, LANES))
        return full, jnp.transpose(full)

    def build_edges(b):
        at = pl.ds(pl.multiple_of(b * LANES, LANES), LANES)
        full, down = across(edst[pl.ds(b, 1), :])
        for c in range(n_node // LANES):
            part = slice(c * LANES, (c + 1) * LANES)
            dd[at, part] = hot(down == lane_i + c * LANES)
            ddt[part, at] = hot(full == sub_i + c * LANES)
        scale = eweight[pl.ds(b, 1), :] * elive[pl.ds(b, 1), :].astype(F32)
        ecol[at, :] = across(scale)[1]
        full, down = across(esrc[pl.ds(b, 1), :])
        for c in range(n_node // LANES):
            part = slice(c * LANES, (c + 1) * LANES)
            so[at, part] = hot(down == lane_i + c * LANES)
            sot[part, at] = hot(full == sub_i + c * LANES)
        for c in range(4 * n_bnd // LANES):
            part = slice(c * LANES, (c + 1) * LANES)
            sr[at, part] = hot(down == lane_i + (n_node + c * LANES))
            srt[part, at] = hot(full == sub_i + (n_node + c * LANES))

    loop(rows_e, build_edges)

    def build_bound(b):
        at = pl.ds(pl.multiple_of(b * LANES, LANES), LANES)
        full, down = across(bidx[pl.ds(b, 1), :])
        for c in range(n_node // LANES):
            part = slice(c * LANES, (c + 1) * LANES)
            bb[at, part] = hot(down == lane_i + c * LANES)
            bbt[part, at] = hot(full == sub_i + c * LANES)

    loop(n_bnd // LANES, build_bound)

    def chunk(c):
        return pl.ds(pl.multiple_of(c * CH, CH), CH)

    def back_last(c):
        at = chunk(c)
        rows = (mm(dd[at, :], cot[...]) * wide(ecol[at, :])).astype(BF)
        gm1[at, :] = rows
        ga1[at, :] = mt(rows, msg_proj[1])

    loop(n_edge // CH, back_last)

    got = pl.ds(0, (n_dev - 1) * TILE)
    cols_done = pltpu.make_async_remote_copy(
        src_ref=rx.at[got, :], dst_ref=rx.at[got, :], send_sem=a2a_send, recv_sem=a2a_recv,
        device_id=(g, o), device_id_type=MESH)
    got_aux = pl.ds(0, n_dev - 1)
    aux_done = pltpu.make_async_remote_copy(
        src_ref=aux_rx.at[got_aux], dst_ref=aux_rx.at[got_aux], send_sem=aux_send, recv_sem=aux_recv,
        device_id=(g, o), device_id_type=MESH)
    cols_done.wait_recv()
    aux_done.wait_recv()
    parts = aux_rx[...].reshape(rows_c, 8, LANES)
    low = jnp.sum(parts[:, 0:4, :], axis=1)
    high = jnp.sum(parts[:, 4:8, :], axis=1)
    srow[...] = jnp.where(lane < 64, low, pltpu.roll(high, 64, axis=1))
    crow[...] = jnp.where(lane < 64, pltpu.roll(low, 64, axis=1), high)

    lane_f = lane_i.astype(F32)
    sub_f = sub_i.astype(F32)

    def build_pool(b):
        at = pl.ds(pl.multiple_of(b * LANES, LANES), LANES)
        full, down = across(srow[pl.ds(b, 1), :])
        for c in range(n_node // LANES):
            part = slice(c * LANES, (c + 1) * LANES)
            pp[at, part] = hot(down == lane_f + float(c * LANES))
            ppt[part, at] = hot(full == sub_f + float(c * LANES))
        ccol[at, :] = across(crow[pl.ds(b, 1), :])[1]

    loop(rows_c, build_pool)

    def sigmoid(v):
        return 0.5 * jnp.tanh(0.5 * v) + 0.5

    def encode(c):
        at = chunk(c)
        v = mm(rx[at, :], enc_in[...])
        s = sigmoid(v)
        a = (v * s).astype(BF)
        eact[at, :] = a
        edsilu[at, :] = s * (1.0 + v * (1.0 - s))
        cemb[at, :] = (mm(a, enc_out[...]) * wide(ccol[at, :])).astype(BF)

    loop(n_col // CH, encode)

    def pool(c):
        at = chunk(c)
        hh[0, at, :] = (static[at, :].astype(F32) + mm(ppt[at, :], cemb[...])).astype(BF)

    loop(n_node // CH, pool)

    def fwd_copy(l, r):
        return pltpu.make_async_remote_copy(
            src_ref=rim_tx.at[l], dst_ref=rim.at[l, r], send_sem=rim_send.at[l, r],
            recv_sem=rim_recv.at[l, r], device_id=near[flip[r]], device_id_type=MESH)

    def back_copy(l, r):
        return pltpu.make_async_remote_copy(
            src_ref=gt_tx.at[l, r], dst_ref=gt_rx.at[l, r], send_sem=gt_send.at[l, r],
            recv_sem=gt_recv.at[l, r], device_id=near[r], device_id_type=MESH)

    def send_rims(l):
        rim_tx[l] = mm(bb[...], hh[l]).astype(BF)
        for r in (2, 3, 0, 1):
            @pl.when(here[flip[r]])
            def _():
                fwd_copy(l, r).start()

    def wait_rims(l):
        for r in range(4):
            @pl.when(here[r])
            def _():
                fwd_copy(l, r).wait_recv()

    def layer_own(l, pre):
        def body(c):
            at = chunk(c)
            h = hh[l]
            xo = mm(so[at, :], h).astype(BF)
            xd = mm(dd[at, :], h).astype(BF)
            pre[at, :] = mm(xo, src_proj[l]) + mm(xd, dst_proj[l])
        loop(n_edge // CH, body)

    def layer_rest(l, pre, act):
        def body(c):
            at = chunk(c)
            xr = mm(sr[at, :], rim[l].reshape(4 * n_bnd, 256)).astype(BF)
            v = pre[at, :] + mm(xr, src_proj[l])
            s = sigmoid(v)
            a = (v * s).astype(BF)
            act[at, :] = a
            slope = s * (1.0 + v * (1.0 - s))
            if l == 0:
                pre[at, :] = slope
            else:
                gp[at, :] = (ga1[at, :] * slope).astype(BF)
            msg[at, :] = (mm(a, msg_proj[l]) * wide(ecol[at, :])).astype(BF)
        loop(n_edge // CH, body)

    def gather_messages(l):
        def body(c):
            at = chunk(c)
            rows = (hh[l, at, :].astype(F32) + mm(ddt[at, :], msg[...])).astype(BF)
            if l == 0:
                hh[1, at, :] = rows
            else:
                node_out[at, :] = rows
        loop(n_node // CH, body)

    send_rims(0)
    layer_own(0, pre0)
    wait_rims(0)
    layer_rest(0, pre0, act0)
    gather_messages(0)
    send_rims(1)
    layer_own(1, pre1)
    wait_rims(1)
    layer_rest(1, pre1, act1)

    def back_rims(l):
        for r in (2, 3, 0, 1):
            rows = mm(srt[r * n_bnd:(r + 1) * n_bnd, :], gp[...]).astype(BF)
            gs_rim[r] = rows
            gt_tx[l, r] = mt(rows, src_proj[l]).astype(BF)

            @pl.when(here[r])
            def _():
                back_copy(l, r).start()

    def back_own(l):
        def body(c):
            at = chunk(c)
            s_rows = mm(sot[at, :], gp[...]).astype(BF)
            d_rows = mm(ddt[at, :], gp[...]).astype(BF)
            gs_own[at, :] = s_rows
            gd[at, :] = d_rows
            before = cot[at, :].astype(F32) if l == 1 else gh[at, :]
            gh[at, :] = before + mt(s_rows, src_proj[l]) + mt(d_rows, dst_proj[l])
        loop(n_node // CH, body)

    def layer_weights(l, act, gm, out):
        total = tm(hh[l], gs_own[...])
        for r in range(4):
            total = total + tm(rim[l, r], gs_rim[r])
        out[0:256, :] = total.astype(BF)
        out[256:512, :] = tm(hh[l], gd[...]).astype(BF)
        acc[...] = jnp.zeros_like(acc)

        def body(c):
            at = chunk(c)
            acc[...] += tm(act[at, :], gm[at, :])
        loop(n_edge // CH, body)
        out[512:768, :] = acc[...].astype(BF)

    def add_rims(l):
        for r in range(4):
            @pl.when(here[flip[r]])
            def _():
                back_copy(l, r).wait_recv()

        def body(c):
            at = chunk(c)
            total = gh[at, :]
            for r in range(4):
                total = total + mm(bbt[at, :], gt_rx[l, r])
            gh[at, :] = total
        loop(n_node // CH, body)

    rounds = ((96, 0, 0), (96, 96, 96), (48, 64, 192))

    def tile_of(k, d):
        return lax.rem(d - rounds[k][1] + n_dev, n_dev)

    def tile_at(ref, t):
        return ref.at[pl.ds(pl.multiple_of((t // 2) * TILE, TILE), TILE),
                      pl.ds(pl.multiple_of(lax.rem(t, 2) * LANES, LANES), LANES)]

    def rs_copy(k, ref, d):
        return pltpu.make_async_remote_copy(
            src_ref=tile_at(ref, tile_of(k, d)), dst_ref=gr.at[k, me], send_sem=rs_send.at[k],
            recv_sem=rs_recv.at[k], device_id=coords(d), device_id_type=MESH)

    def scatter_start(k, ref):
        count = rounds[k][0]

        def one(d):
            @pl.when(tile_of(k, d) < count)
            def _():
                rs_copy(k, ref, d).start()
        others(one)

        @pl.when(tile_of(k, me) < count)
        def _():
            t = tile_of(k, me)
            gr[k, me] = ref[pl.ds(pl.multiple_of((t // 2) * TILE, TILE), TILE),
                            pl.ds(pl.multiple_of(lax.rem(t, 2) * LANES, LANES), LANES)]

    def span_wait(k, n, sems, what):
        at = pl.ds(0, n)
        copy = pltpu.make_async_remote_copy(
            src_ref=gr.at[k, at], dst_ref=gr.at[k, at], send_sem=sems.at[k], recv_sem=sems.at[k],
            device_id=(g, o), device_id_type=MESH)
        if what == "recv":
            copy.wait_recv()
        else:
            copy.wait_send()

    def ag_copy(k, d):
        return pltpu.make_async_remote_copy(
            src_ref=ag.at[k], dst_ref=gall.at[rounds[k][2] + tile_of(k, me)], send_sem=ag_send.at[k],
            recv_sem=ag_recv.at[k], device_id=coords(d), device_id_type=MESH)

    def own_copy(k):
        return pltpu.make_async_copy(ag.at[k], gall.at[rounds[k][2] + tile_of(k, me)], own_sem.at[k])

    def gather_start(k):
        @pl.when(tile_of(k, me) < rounds[k][0])
        def _():
            span_wait(k, n_dev - 1, rs_recv, "recv")

            def body(s, total):
                for i in range(8):
                    total = total + gr[k, s * 8 + i].astype(F32)
                return total
            total = lax.fori_loop(0, n_dev // 8, body, jnp.zeros((TILE, LANES), F32))
            ag[k] = total.astype(BF)
            own_copy(k).start()
            others(lambda d: ag_copy(k, d).start())

    def finish(k):
        count = rounds[k][0]

        @pl.when(tile_of(k, me) < count)
        def _():
            own_copy(k).wait()
            span_wait(k, count - 1, rs_send, "send")
            span_wait(k, n_dev - 1, ag_send, "send")
            at = pl.ds(0, count - 1)
            pltpu.make_async_remote_copy(
                src_ref=gall.at[at], dst_ref=gall.at[at], send_sem=ag_send.at[k],
                recv_sem=ag_recv.at[k], device_id=(g, o), device_id_type=MESH).wait_recv()

        @pl.when(tile_of(k, me) >= count)
        def _():
            span_wait(k, count, rs_send, "send")
            at = pl.ds(0, count)
            pltpu.make_async_remote_copy(
                src_ref=gall.at[at], dst_ref=gall.at[at], send_sem=ag_send.at[k],
                recv_sem=ag_recv.at[k], device_id=(g, o), device_id_type=MESH).wait_recv()

    back_rims(1)
    back_own(1)
    layer_weights(1, act1, gm1, g1)
    scatter_start(0, g1)
    gather_messages(1)
    add_rims(1)

    def back_first(c):
        at = chunk(c)
        rows = (mm(dd[at, :], gh[...].astype(BF)) * wide(ecol[at, :])).astype(BF)
        gm0[at, :] = rows
        gp[at, :] = (mt(rows, msg_proj[0]) * pre0[at, :]).astype(BF)

    loop(n_edge // CH, back_first)
    back_rims(0)
    back_own(0)
    layer_weights(0, act0, gm0, g0)
    scatter_start(1, g0)
    gather_start(0)
    add_rims(0)

    ge[0:256, :] = jnp.zeros((256, 256), BF)
    acc[...] = jnp.zeros_like(acc)

    def encode_out(c):
        at = chunk(c)
        rows = (mm(pp[at, :], gh[...].astype(BF)) * wide(ccol[at, :])).astype(BF)
        acc[...] += tm(eact[at, :], rows)
        cemb[at, :] = (mt(rows, enc_out[...]) * edsilu[at, :]).astype(BF)

    loop(n_col // CH, encode_out)
    ge[0:256, :] = acc[...].astype(BF)
    acc[...] = jnp.zeros_like(acc)

    def encode_in(c):
        at = chunk(c)
        acc[0:128, :] += tm(rx[at, :], cemb[at, :])

    loop(n_col // CH, encode_in)
    ge[256:384, :] = acc[0:128, :].astype(BF)
    scatter_start(2, ge)
    gather_start(1)
    gather_start(2)

    cols_done.wait_send()
    aux_done.wait_send()
    for l in range(2):
        for r in range(4):
            @pl.when(here[flip[r]])
            def _():
                fwd_copy(l, r).wait_send()

            @pl.when(here[r])
            def _():
                back_copy(l, r).wait_send()
    for k in range(3):
        finish(k)


def finish_kernel(gall, node_in, enc_in_g, enc_out_g, src_g, dst_g, msg_g, node_out):
    node_out[...] = node_in[...]
    layer_refs = (src_g, dst_g, msg_g)

    def put(first, count, store):
        for t in range(count):
            rb, half = t // 2, t % 2
            rows = slice(rb * TILE, (rb + 1) * TILE)
            store(rows, slice(half * LANES, (half + 1) * LANES), gall[first + t].astype(F32))

    for layer, first in ((1, 0), (0, 96)):
        for m in range(3):
            def store(rows, lanes, v, ref=layer_refs[m], layer=layer):
                ref[layer, rows, lanes] = v
            put(first + 32 * m, 32, store)

    def store_out(rows, lanes, v):
        enc_out_g[rows, lanes] = v

    def store_in(rows, lanes, v):
        enc_in_g[rows, lanes] = v

    put(192, 32, store_out)
    put(224, 16, store_in)


def per_device(n_grid, n_dom, columns, column_live, col_weight, col_slot, node_static, boundary_idx,
               edge_src, edge_dst, edge_live, edge_weight, enc_in, enc_out, src_proj, dst_proj, msg_proj,
               node_cotangent):
    n_dev = n_grid * n_dom
    n_col = columns.shape[0]
    n_edge = edge_src.shape[0]
    n_node, width = node_static.shape
    n_bnd = boundary_idx.shape[0]
    rows = lambda x: x.reshape(-1, LANES)
    vm = lambda *shape: pltpu.VMEM(shape, BF)
    vf = lambda *shape: pltpu.VMEM(shape, F32)
    dma = pltpu.SemaphoreType.DMA
    scratch = [
        vf(n_dev, LANES), vf(n_dev, LANES), vm(n_col, columns.shape[1]), vf(n_col // LANES, LANES),
        vf(n_col // LANES, LANES), vf(n_col, LANES), vf(n_edge, LANES),
        vm(n_edge, n_node), vm(n_edge, 4 * n_bnd), vm(n_node, n_edge), vm(4 * n_bnd, n_edge),
        vm(n_edge, n_node), vm(n_node, n_edge), vm(n_bnd, n_node), vm(n_node, n_bnd),
        vm(n_col, n_node), vm(n_node, n_col),
        vm(2, n_node, width), vm(2, 4, n_bnd, width), vm(2, n_bnd, width), vm(2, 4, n_bnd, width),
        vm(2, 4, n_bnd, width),
        vm(n_col, width), vf(n_col, width), vm(n_col, width), vf(n_edge, width), vf(n_edge, width),
        vm(n_edge, width), vm(n_edge, width), vm(n_edge, width), vm(n_edge, width), vm(n_edge, width),
        vf(n_edge, width), vm(n_edge, width), vm(n_node, width), vm(4, n_bnd, width), vm(n_node, width),
        vf(n_node, width),
        vf(width, width), vm(768, width), vm(768, width), vm(384, width), vm(3, n_dev, TILE, LANES),
        vm(3, TILE, LANES),
        dma(()), dma(()), dma(()), dma(()), dma((2, 4)), dma((2, 4)), dma((2, 4)), dma((2, 4)),
        dma((3,)), dma((3,)), dma((3,)), dma((3,)), dma((3,)),
    ]
    in_vmem = pl.BlockSpec(memory_space=pltpu.VMEM)
    node_out, gall = pl.pallas_call(
        functools.partial(step_kernel, n_grid, n_dom),
        out_shape=(jax.ShapeDtypeStruct((n_node, width), BF), jax.ShapeDtypeStruct((240, TILE, LANES), BF)),
        in_specs=[in_vmem] * 16,
        out_specs=(in_vmem, pl.BlockSpec(memory_space=pl.ANY)),
        scratch_shapes=scratch,
        compiler_params=pltpu.CompilerParams(
            collective_id=0, has_side_effects=True, vmem_limit_bytes=62 * 1024 * 1024),
    )(columns, rows(column_live), rows(col_weight), rows(col_slot), node_static, rows(boundary_idx),
      rows(edge_src), rows(edge_dst), rows(edge_live), rows(edge_weight), enc_in, enc_out, src_proj,
      dst_proj, msg_proj, node_cotangent)
    mat = jax.ShapeDtypeStruct((width, width), F32)
    pair = jax.ShapeDtypeStruct((2, width, width), F32)
    enc_in_g, enc_out_g, src_g, dst_g, msg_g, node_final = pl.pallas_call(
        finish_kernel,
        out_shape=(jax.ShapeDtypeStruct(enc_in.shape, F32), mat, pair, pair, pair,
                   jax.ShapeDtypeStruct((n_node, width), BF)),
        in_specs=[in_vmem] * 2,
        out_specs=(in_vmem,) * 6,
    )(gall, node_out)
    return (node_final, enc_in_g, enc_out_g, src_g, dst_g, msg_g)


def solution(mesh):
    n_grid, n_dom = mesh.shape["grid"], mesh.shape["dom"]
    both = P(("grid", "dom"))
    rows = P(("grid", "dom"), None)
    placed = (rows, both, both, both, rows, both, both, both, both, both, P(), P(), P(), P(), P(), rows)
    return jax.shard_map(
        functools.partial(per_device, n_grid, n_dom),
        mesh=mesh,
        in_specs=placed,
        out_specs=(rows, P(), P(), P(), P(), P()),
        check_vma=False,
    )
```

```python
import functools

import jax
import jax.numpy as jnp
from jax import lax
from jax.experimental import pallas as pl
from jax.experimental.pallas import tpu as pltpu
from jax.sharding import PartitionSpec as P

MESH = pl.DeviceIdType.MESH
BF = jnp.bfloat16
F32 = jnp.float32
CH = 512
LANES = 128
TILE = 16


def mm(a, b):
    return lax.dot_general(a, b, (((1,), (0,)), ((), ())), preferred_element_type=F32)


def mt(a, b):
    return lax.dot_general(a, b, (((1,), (1,)), ((), ())), preferred_element_type=F32)


def tm(a, b):
    return lax.dot_general(a, b, (((0,), (0,)), ((), ())), preferred_element_type=F32)


def wide(x):
    return jnp.concatenate([x, x], axis=1)


def hot(equal):
    return jnp.where(equal, 1.0, 0.0).astype(BF)


def step_kernel(
    n_grid, n_dom,
    n_in, *refs,
):
    inputs = refs[:n_in]
    node_out, gall = refs[n_in:n_in + 2]
    copies = refs[n_in + 2:2 * n_in + 2]
    step_body(n_grid, n_dom, inputs, copies, node_out, gall, *refs[2 * n_in + 2:])


def step_body(
    n_grid, n_dom, inputs, copies, node_out, gall,
    in_sem, round_sem, aux_tx, aux_rx, rx, srow, crow, ccol, ecol,
    so, sr, sot, srt, dd, ddt, bb, bbt, pp, ppt,
    hh, rim, rim_tx, gt_tx, gt_rx,
    eact, edsilu, cemb, pre0, pre1, act0, act1, msg, gm0, gm1, ga1, gp, gs_own, gs_rim, gd, gh,
    acc, g1, g0, ge, px1, px0, pxe, tx1, tx0, txe, gr, ag,
    pair_send, pair_recv,
    a2a_send, a2a_recv, aux_send, aux_recv, rim_send, rim_recv, gt_send, gt_recv,
    rs_send, rs_recv, ag_send, ag_recv, own_sem,
):
    (cols, live, cweight, slot, static, bidx, esrc, edst, elive, eweight,
     enc_in, enc_out, src_proj, dst_proj, msg_proj, cot) = copies
    n_dev = n_grid * n_dom
    n_node = static.shape[0]
    n_edge = so.shape[0]
    n_col = cols.shape[0]
    n_bnd = bb.shape[0]
    rows_e = n_edge // LANES
    rows_c = n_col // LANES
    g = lax.axis_index("grid")
    o = lax.axis_index("dom")
    me = g * n_dom + o

    core = lax.rem(g, 2)
    z = g // 2
    n_z, n_y, n_x = n_grid // 2, n_dom // 4, 4
    y, x = o // n_x, lax.rem(o, n_x)
    chip = z * n_dom + o
    n_chip = n_dev // 2

    def others(fn, cores=(1, 0)):
        def some(i, skip):
            to_z = lax.rem(z + (n_z - 1 - i // n_y), n_z)
            to_y = lax.rem(y + (n_y - 1 - lax.rem(i, n_y)), n_y)
            for dx in (2, 1, 3, 0):
                to_o = to_y * n_x + lax.rem(x + dx, n_x)
                for dc in cores:
                    if not (skip and dx == 0 and dc == 0):
                        fn(to_z * 2 + (1 - core if dc else core), to_o)

        def body(i, carry):
            some(i, False)
            return carry
        lax.fori_loop(0, n_z * n_y - 1, body, 0)
        some(n_z * n_y - 1, True)

    def loop(n, fn):
        def body(k, carry):
            fn(k)
            return carry
        lax.fori_loop(0, n, body, 0)

    def load(i):
        return pltpu.make_async_copy(inputs[i], copies[i], in_sem.at[i])

    barrier = pltpu.get_barrier_semaphore()

    def column(fn):
        for k in range(1, n_grid):
            fn((lax.rem(g + k, n_grid), o))

    def greet(sem, to):
        pl.semaphore_signal(sem, inc=1, device_id=to, device_id_type=MESH)

    for k in range(1, n_dom):
        greet(barrier, (g, lax.rem(o + k, n_dom)))
    column(lambda to: greet(barrier, to))
    order = (0, 1, 2, 3, 6, 7, 8, 9, 5, 15, 14, 10, 11, 4, 12, 13)
    for i in order:
        load(i).start()
    for i in order[:4]:
        load(i).wait()

    lane = lax.broadcasted_iota(jnp.int32, (rows_c, LANES), 1)
    quarter = lax.rem(me, 4)
    slot_f = slot[...].astype(F32)
    scale_f = cweight[...] * live[...].astype(F32)
    for j in range(8):
        to_slot = lax.rem((quarter - j) * 16 + 2 * LANES, LANES)
        to_scale = lax.rem((quarter - j) * 16 + 64 + 2 * LANES, LANES)
        a = pltpu.roll(slot_f, to_slot, axis=1)
        b = pltpu.roll(scale_f, to_scale, axis=1)
        row = jnp.where(lane // 16 == quarter, a, jnp.where(lane // 16 == quarter + 4, b, 0.0))
        aux_tx[pl.ds(j, rows_c, stride=8), :] = row

    pl.semaphore_wait(barrier, n_dom + n_grid - 2)
    column(lambda to: greet(round_sem, to))
    pl.semaphore_wait(round_sem, n_grid - 1)

    def send_aux(to_g, to_o):
        d = to_g * n_dom + to_o
        pltpu.make_async_remote_copy(
            src_ref=aux_tx.at[d], dst_ref=aux_rx.at[me],
            send_sem=aux_send, recv_sem=aux_recv, device_id=(to_g, to_o), device_id_type=MESH,
        ).start()

    def send_cols(to_g, to_o):
        d = to_g * n_dom + to_o
        pltpu.make_async_remote_copy(
            src_ref=cols.at[pl.ds(pl.multiple_of(d * TILE, TILE), TILE), :],
            dst_ref=rx.at[pl.ds(pl.multiple_of(me * TILE, TILE), TILE), :],
            send_sem=a2a_send, recv_sem=a2a_recv, device_id=(to_g, to_o), device_id_type=MESH,
        ).start()

    others(send_aux)
    others(send_cols)
    for i in order[4:]:
        load(i).wait()
    mine = pl.ds(pl.multiple_of(me * TILE, TILE), TILE)
    rx[mine, :] = cols[mine, :]
    aux_rx[me] = aux_tx[me]

    here = (g > 0, g < n_grid - 1, o > 0, o < n_dom - 1)
    near = ((g - 1, o), (g + 1, o), (g, o - 1), (g, o + 1))
    flip = (1, 0, 3, 2)
    for r in range(4):
        @pl.when(jnp.logical_not(here[r]))
        def _():
            for l in range(2):
                rim[l, r] = jnp.zeros((n_bnd, 256), BF)
                gt_rx[l, flip[r]] = jnp.zeros((n_bnd, 256), BF)

    lane_i = lax.broadcasted_iota(jnp.int32, (LANES, LANES), 1)
    sub_i = lax.broadcasted_iota(jnp.int32, (LANES, LANES), 0)

    def across(row):
        full = jnp.broadcast_to(row, (LANES, LANES))
        return full, jnp.transpose(full)

    def build_edges(b):
        at = pl.ds(pl.multiple_of(b * LANES, LANES), LANES)
        full, down = across(edst[pl.ds(b, 1), :])
        for c in range(n_node // LANES):
            part = slice(c * LANES, (c + 1) * LANES)
            dd[at, part] = hot(down == lane_i + c * LANES)
            ddt[part, at] = hot(full == sub_i + c * LANES)
        scale = eweight[pl.ds(b, 1), :] * elive[pl.ds(b, 1), :].astype(F32)
        ecol[at, :] = across(scale)[1]
        full, down = across(esrc[pl.ds(b, 1), :])
        for c in range(n_node // LANES):
            part = slice(c * LANES, (c + 1) * LANES)
            so[at, part] = hot(down == lane_i + c * LANES)
            sot[part, at] = hot(full == sub_i + c * LANES)
        for c in range(4 * n_bnd // LANES):
            part = slice(c * LANES, (c + 1) * LANES)
            sr[at, part] = hot(down == lane_i + (n_node + c * LANES))
            srt[part, at] = hot(full == sub_i + (n_node + c * LANES))

    loop(rows_e, build_edges)

    def build_bound(b):
        at = pl.ds(pl.multiple_of(b * LANES, LANES), LANES)
        full, down = across(bidx[pl.ds(b, 1), :])
        for c in range(n_node // LANES):
            part = slice(c * LANES, (c + 1) * LANES)
            bb[at, part] = hot(down == lane_i + c * LANES)
            bbt[part, at] = hot(full == sub_i + c * LANES)

    loop(n_bnd // LANES, build_bound)

    def chunk(c):
        return pl.ds(pl.multiple_of(c * CH, CH), CH)

    def back_last(c):
        at = chunk(c)
        rows = (mm(dd[at, :], cot[...]) * wide(ecol[at, :])).astype(BF)
        gm1[at, :] = rows
        ga1[at, :] = mt(rows, msg_proj[1])

    loop(n_edge // CH, back_last)

    got = pl.ds(0, (n_dev - 1) * TILE)
    cols_done = pltpu.make_async_remote_copy(
        src_ref=rx.at[got, :], dst_ref=rx.at[got, :], send_sem=a2a_send, recv_sem=a2a_recv,
        device_id=(g, o), device_id_type=MESH)
    got_aux = pl.ds(0, n_dev - 1)
    aux_done = pltpu.make_async_remote_copy(
        src_ref=aux_rx.at[got_aux], dst_ref=aux_rx.at[got_aux], send_sem=aux_send, recv_sem=aux_recv,
        device_id=(g, o), device_id_type=MESH)
    aux_done.wait_recv()
    parts = aux_rx[...].reshape(rows_c, 8, LANES)
    low = jnp.sum(parts[:, 0:4, :], axis=1)
    high = jnp.sum(parts[:, 4:8, :], axis=1)
    srow[...] = jnp.where(lane < 64, low, pltpu.roll(high, 64, axis=1))
    crow[...] = jnp.where(lane < 64, pltpu.roll(low, 64, axis=1), high)

    lane_f = lane_i.astype(F32)
    sub_f = sub_i.astype(F32)

    def build_pool(b):
        at = pl.ds(pl.multiple_of(b * LANES, LANES), LANES)
        full, down = across(srow[pl.ds(b, 1), :])
        for c in range(n_node // LANES):
            part = slice(c * LANES, (c + 1) * LANES)
            pp[at, part] = hot(down == lane_f + float(c * LANES))
            ppt[part, at] = hot(full == sub_f + float(c * LANES))
        ccol[at, :] = across(crow[pl.ds(b, 1), :])[1]

    loop(rows_c, build_pool)
    cols_done.wait_recv()

    def sigmoid(v):
        return 0.5 * jnp.tanh(0.5 * v) + 0.5

    def encode(c):
        at = chunk(c)
        v = mm(rx[at, :], enc_in[...])
        s = sigmoid(v)
        a = (v * s).astype(BF)
        eact[at, :] = a
        edsilu[at, :] = s * (1.0 + v * (1.0 - s))
        cemb[at, :] = (mm(a, enc_out[...]) * wide(ccol[at, :])).astype(BF)

    loop(n_col // CH, encode)

    def pool(c):
        at = chunk(c)
        hh[0, at, :] = (static[at, :].astype(F32) + mm(ppt[at, :], cemb[...])).astype(BF)

    loop(n_node // CH, pool)

    def fwd_copy(l, r):
        return pltpu.make_async_remote_copy(
            src_ref=rim_tx.at[l], dst_ref=rim.at[l, r], send_sem=rim_send.at[l, r],
            recv_sem=rim_recv.at[l, r], device_id=near[flip[r]], device_id_type=MESH)

    def back_copy(l, r):
        return pltpu.make_async_remote_copy(
            src_ref=gt_tx.at[l, r], dst_ref=gt_rx.at[l, r], send_sem=gt_send.at[l, r],
            recv_sem=gt_recv.at[l, r], device_id=near[r], device_id_type=MESH)

    def send_rims(l):
        rim_tx[l] = mm(bb[...], hh[l]).astype(BF)
        for r in (2, 3, 0, 1):
            @pl.when(here[flip[r]])
            def _():
                fwd_copy(l, r).start()

    def wait_rims(l):
        for r in range(4):
            @pl.when(here[r])
            def _():
                fwd_copy(l, r).wait_recv()

    def layer_own(l, pre):
        def body(c):
            at = chunk(c)
            h = hh[l]
            xo = mm(so[at, :], h).astype(BF)
            xd = mm(dd[at, :], h).astype(BF)
            pre[at, :] = mm(xo, src_proj[l]) + mm(xd, dst_proj[l])
        loop(n_edge // CH, body)

    def layer_rest(l, pre, act):
        def body(c):
            at = chunk(c)
            xr = mm(sr[at, :], rim[l].reshape(4 * n_bnd, 256)).astype(BF)
            v = pre[at, :] + mm(xr, src_proj[l])
            s = sigmoid(v)
            a = (v * s).astype(BF)
            act[at, :] = a
            slope = s * (1.0 + v * (1.0 - s))
            if l == 0:
                pre[at, :] = slope
            else:
                gp[at, :] = (ga1[at, :] * slope).astype(BF)
            msg[at, :] = (mm(a, msg_proj[l]) * wide(ecol[at, :])).astype(BF)
        loop(n_edge // CH, body)

    def gather_messages(l):
        def body(c):
            at = chunk(c)
            rows = (hh[l, at, :].astype(F32) + mm(ddt[at, :], msg[...])).astype(BF)
            if l == 0:
                hh[1, at, :] = rows
            else:
                node_out[at, :] = rows
        loop(n_node // CH, body)

    send_rims(0)
    layer_own(0, pre0)
    wait_rims(0)
    layer_rest(0, pre0, act0)
    gather_messages(0)
    send_rims(1)
    layer_own(1, pre1)
    wait_rims(1)
    layer_rest(1, pre1, act1)

    def back_rims(l):
        for r in (2, 3, 0, 1):
            rows = mm(srt[r * n_bnd:(r + 1) * n_bnd, :], gp[...]).astype(BF)
            gs_rim[r] = rows
            gt_tx[l, r] = mt(rows, src_proj[l]).astype(BF)

            @pl.when(here[r])
            def _():
                back_copy(l, r).start()

    def back_own(l):
        def body(c):
            at = chunk(c)
            s_rows = mm(sot[at, :], gp[...]).astype(BF)
            d_rows = mm(ddt[at, :], gp[...]).astype(BF)
            gs_own[at, :] = s_rows
            gd[at, :] = d_rows
            before = cot[at, :].astype(F32) if l == 1 else gh[at, :]
            gh[at, :] = before + mt(s_rows, src_proj[l]) + mt(d_rows, dst_proj[l])
        loop(n_node // CH, body)

    def halves(out, first, value):
        rows = slice(first, first + value.shape[0])
        out[0, rows, :] = value[:, 0:LANES]
        out[1, rows, :] = value[:, LANES:]

    def layer_weights(l, act, gm, out):
        total = tm(hh[l], gs_own[...])
        for r in range(4):
            total = total + tm(rim[l, r], gs_rim[r])
        halves(out, 0, total)
        halves(out, 256, tm(hh[l], gd[...]))
        acc[...] = jnp.zeros_like(acc)

        def body(c):
            at = chunk(c)
            acc[...] += tm(act[at, :], gm[at, :])
        loop(n_edge // CH, body)
        halves(out, 512, acc[...])

    def add_rims(l):
        for r in range(4):
            @pl.when(here[flip[r]])
            def _():
                back_copy(l, r).wait_recv()

        def body(c):
            at = chunk(c)
            total = gh[at, :]
            for r in range(4):
                total = total + mm(bbt[at, :], gt_rx[l, r])
            gh[at, :] = total
        loop(n_node // CH, body)

    rounds = ((48, 0, 0), (48, 48, 48), (24, 32, 96))
    parts_of = ((g1, px1, tx1), (g0, px0, tx0), (ge, pxe, txe))

    def tile_of(k, q):
        return lax.rem(q - rounds[k][1] + n_chip, n_chip)

    def pair_copy(k):
        mine, theirs, _ = parts_of[k]
        return pltpu.make_async_remote_copy(
            src_ref=mine.at[1 - core], dst_ref=theirs, send_sem=pair_send.at[k],
            recv_sem=pair_recv.at[k], device_id=(g + 1 - 2 * core, o), device_id_type=MESH)

    def rows_of(t):
        return pl.ds(pl.multiple_of(t * TILE, TILE), TILE)

    def scatter_start(k):
        count = rounds[k][0]
        mine, theirs, out = parts_of[k]
        pair_copy(k).wait_recv()

        def add(c):
            at = pl.ds(pl.multiple_of(c * LANES, LANES), LANES)
            out[at, :] = (mine[core, at, :] + theirs[at, :]).astype(BF)
        loop(out.shape[0] // LANES, add)

        def one(to_g, to_o):
            t = tile_of(k, (to_g // 2) * n_dom + to_o)

            @pl.when(t < count)
            def _():
                pltpu.make_async_remote_copy(
                    src_ref=out.at[rows_of(t), :], dst_ref=gr.at[k, chip], send_sem=rs_send.at[k],
                    recv_sem=rs_recv.at[k], device_id=(to_g, to_o), device_id_type=MESH).start()
        others(one, cores=(0,))

        @pl.when(tile_of(k, chip) < count)
        def _():
            gr[k, chip] = out[rows_of(tile_of(k, chip)), :]

    def span_wait(ref, n, sem, what):
        at = pl.ds(0, n)
        copy = pltpu.make_async_remote_copy(
            src_ref=ref.at[at], dst_ref=ref.at[at], send_sem=sem, recv_sem=sem,
            device_id=(g, o), device_id_type=MESH)
        if what == "recv":
            copy.wait_recv()
        else:
            copy.wait_send()

    def place(k):
        return gall.at[2 * (rounds[k][2] + tile_of(k, chip)) + core]

    def own_copy(k):
        return pltpu.make_async_copy(ag.at[k], place(k), own_sem.at[k])

    def gather_start(k):
        @pl.when(tile_of(k, chip) < rounds[k][0])
        def _():
            span_wait(gr.at[k], n_chip - 1, rs_recv.at[k], "recv")

            def body(s, total):
                for i in range(8):
                    total = total + gr[k, s * 8 + i].astype(F32)
                return total
            total = lax.fori_loop(0, n_chip // 8, body, jnp.zeros((TILE, LANES), F32))
            ag[k] = total.astype(BF)
            own_copy(k).start()

            def one(to_g, to_o):
                pltpu.make_async_remote_copy(
                    src_ref=ag.at[k], dst_ref=place(k), send_sem=ag_send.at[k],
                    recv_sem=ag_recv.at[k], device_id=(to_g, to_o), device_id_type=MESH).start()
            others(one)

    def finish(k):
        count = rounds[k][0]
        pair_copy(k).wait_send()

        @pl.when(tile_of(k, chip) < count)
        def _():
            own_copy(k).wait()
            span_wait(gr.at[k], count - 1, rs_send.at[k], "send")
            span_wait(gall, n_dev - 1, ag_send.at[k], "send")
            span_wait(gall, 2 * count - 1, ag_recv.at[k], "recv")

        @pl.when(tile_of(k, chip) >= count)
        def _():
            span_wait(gr.at[k], count, rs_send.at[k], "send")
            span_wait(gall, 2 * count, ag_recv.at[k], "recv")

    back_rims(1)
    back_own(1)
    layer_weights(1, act1, gm1, g1)
    pair_copy(0).start()
    gather_messages(1)
    scatter_start(0)
    add_rims(1)

    def back_first(c):
        at = chunk(c)
        rows = (mm(dd[at, :], gh[...].astype(BF)) * wide(ecol[at, :])).astype(BF)
        gm0[at, :] = rows
        gp[at, :] = (mt(rows, msg_proj[0]) * pre0[at, :]).astype(BF)

    loop(n_edge // CH, back_first)
    back_rims(0)
    gather_start(0)
    back_own(0)
    layer_weights(0, act0, gm0, g0)
    pair_copy(1).start()
    scatter_start(1)
    add_rims(0)

    acc[...] = jnp.zeros_like(acc)

    def encode_out(c):
        at = chunk(c)
        rows = (mm(pp[at, :], gh[...].astype(BF)) * wide(ccol[at, :])).astype(BF)
        acc[...] += tm(eact[at, :], rows)
        cemb[at, :] = (mt(rows, enc_out[...]) * edsilu[at, :]).astype(BF)

    loop(n_col // CH, encode_out)
    halves(ge, 0, acc[...])
    acc[...] = jnp.zeros_like(acc)

    def encode_in(c):
        at = chunk(c)
        acc[0:128, :] += tm(rx[at, :], cemb[at, :])

    loop(n_col // CH, encode_in)
    halves(ge, 256, acc[0:128, :])
    pair_copy(2).start()
    gather_start(1)
    scatter_start(2)
    gather_start(2)

    cols_done.wait_send()
    aux_done.wait_send()
    for l in range(2):
        for r in range(4):
            @pl.when(here[flip[r]])
            def _():
                fwd_copy(l, r).wait_send()

            @pl.when(here[r])
            def _():
                back_copy(l, r).wait_send()
    for k in range(3):
        finish(k)


def finish_kernel(gall, node_in, enc_in_g, enc_out_g, src_g, dst_g, msg_g, node_out):
    node_out[...] = node_in[...]
    layer_refs = (src_g, dst_g, msg_g)

    def put(first, count, store):
        for t in range(count):
            rb, half = t // 2, t % 2
            rows = slice(rb * TILE, (rb + 1) * TILE)
            store(rows, slice(half * LANES, (half + 1) * LANES), gall[first + t].astype(F32))

    for layer, first in ((1, 0), (0, 96)):
        for m in range(3):
            def store(rows, lanes, v, ref=layer_refs[m], layer=layer):
                ref[layer, rows, lanes] = v
            put(first + 32 * m, 32, store)

    def store_out(rows, lanes, v):
        enc_out_g[rows, lanes] = v

    def store_in(rows, lanes, v):
        enc_in_g[rows, lanes] = v

    put(192, 32, store_out)
    put(224, 16, store_in)


def per_device(n_grid, n_dom, columns, column_live, col_weight, col_slot, node_static, boundary_idx,
               edge_src, edge_dst, edge_live, edge_weight, enc_in, enc_out, src_proj, dst_proj, msg_proj,
               node_cotangent):
    n_dev = n_grid * n_dom
    n_col = columns.shape[0]
    n_edge = edge_src.shape[0]
    n_node, width = node_static.shape
    n_bnd = boundary_idx.shape[0]
    rows = lambda x: x.reshape(-1, LANES)
    vm = lambda *shape: pltpu.VMEM(shape, BF)
    vf = lambda *shape: pltpu.VMEM(shape, F32)
    dma = pltpu.SemaphoreType.DMA
    args = (columns, rows(column_live), rows(col_weight), rows(col_slot), node_static, rows(boundary_idx),
            rows(edge_src), rows(edge_dst), rows(edge_live), rows(edge_weight), enc_in, enc_out, src_proj,
            dst_proj, msg_proj, node_cotangent)
    scratch = [pltpu.VMEM(a.shape, a.dtype) for a in args] + [
        dma((len(args),)), pltpu.SemaphoreType.REGULAR,
        vf(n_dev, LANES), vf(n_dev, LANES), vm(n_col, columns.shape[1]), vf(n_col // LANES, LANES),
        vf(n_col // LANES, LANES), vf(n_col, LANES), vf(n_edge, LANES),
        vm(n_edge, n_node), vm(n_edge, 4 * n_bnd), vm(n_node, n_edge), vm(4 * n_bnd, n_edge),
        vm(n_edge, n_node), vm(n_node, n_edge), vm(n_bnd, n_node), vm(n_node, n_bnd),
        vm(n_col, n_node), vm(n_node, n_col),
        vm(2, n_node, width), vm(2, 4, n_bnd, width), vm(2, n_bnd, width), vm(2, 4, n_bnd, width),
        vm(2, 4, n_bnd, width),
        vm(n_col, width), vf(n_col, width), vm(n_col, width), vf(n_edge, width), vf(n_edge, width),
        vm(n_edge, width), vm(n_edge, width), vm(n_edge, width), vm(n_edge, width), vm(n_edge, width),
        vf(n_edge, width), vm(n_edge, width), vm(n_node, width), vm(4, n_bnd, width), vm(n_node, width),
        vf(n_node, width),
        vf(width, width), vf(2, 768, LANES), vf(2, 768, LANES), vf(2, 384, LANES),
        vf(768, LANES), vf(768, LANES), vf(384, LANES), vm(768, LANES), vm(768, LANES), vm(384, LANES),
        vm(3, n_dev // 2, TILE, LANES), vm(3, TILE, LANES), dma((3,)), dma((3,)),
        dma(()), dma(()), dma(()), dma(()), dma((2, 4)), dma((2, 4)), dma((2, 4)), dma((2, 4)),
        dma((3,)), dma((3,)), dma((3,)), dma((3,)), dma((3,)),
    ]
    in_vmem = pl.BlockSpec(memory_space=pltpu.VMEM)
    node_out, gall = pl.pallas_call(
        functools.partial(step_kernel, n_grid, n_dom, len(args)),
        out_shape=(jax.ShapeDtypeStruct((n_node, width), BF), jax.ShapeDtypeStruct((240, TILE, LANES), BF)),
        in_specs=[pl.BlockSpec(memory_space=pl.ANY)] * len(args),
        out_specs=(in_vmem, pl.BlockSpec(memory_space=pl.ANY)),
        scratch_shapes=scratch,
        compiler_params=pltpu.CompilerParams(
            collective_id=0, has_side_effects=True, vmem_limit_bytes=62 * 1024 * 1024),
    )(*args)
    mat = jax.ShapeDtypeStruct((width, width), F32)
    pair = jax.ShapeDtypeStruct((2, width, width), F32)
    enc_in_g, enc_out_g, src_g, dst_g, msg_g, node_final = pl.pallas_call(
        finish_kernel,
        out_shape=(jax.ShapeDtypeStruct(enc_in.shape, F32), mat, pair, pair, pair,
                   jax.ShapeDtypeStruct((n_node, width), BF)),
        in_specs=[in_vmem] * 2,
        out_specs=(in_vmem,) * 6,
    )(gall, node_out)
    return (node_final, enc_in_g, enc_out_g, src_g, dst_g, msg_g)


def solution(mesh):
    n_grid, n_dom = mesh.shape["grid"], mesh.shape["dom"]
    both = P(("grid", "dom"))
    rows = P(("grid", "dom"), None)
    placed = (rows, both, both, both, rows, both, both, both, both, both, P(), P(), P(), P(), P(), rows)
    return jax.shard_map(
        functools.partial(per_device, n_grid, n_dom),
        mesh=mesh,
        in_specs=placed,
        out_specs=(rows, P(), P(), P(), P(), P()),
        check_vma=False,
    )
```

```python
import functools

import jax
import jax.numpy as jnp
from jax import lax
from jax.experimental import pallas as pl
from jax.experimental.pallas import tpu as pltpu
from jax.sharding import PartitionSpec as P

MESH = pl.DeviceIdType.MESH
BF = jnp.bfloat16
F32 = jnp.float32
CH = 1024
CN = 512
LANES = 128
TILE = 16


def mm(a, b):
    return lax.dot_general(a, b, (((1,), (0,)), ((), ())), preferred_element_type=F32)


def mt(a, b):
    return lax.dot_general(a, b, (((1,), (1,)), ((), ())), preferred_element_type=F32)


def tm(a, b):
    return lax.dot_general(a, b, (((0,), (0,)), ((), ())), preferred_element_type=F32)


def wide(x):
    return jnp.concatenate([x, x], axis=1)


def hot(equal):
    return jnp.where(equal, 1.0, 0.0).astype(BF)


def step_kernel(
    n_grid, n_dom,
    n_in, *refs,
):
    inputs = refs[:n_in]
    node_out, gall = refs[n_in:n_in + 2]
    copies = refs[n_in + 2:2 * n_in + 2]
    step_body(n_grid, n_dom, inputs, copies, node_out, gall, *refs[2 * n_in + 2:])


def step_body(
    n_grid, n_dom, inputs, copies, node_out, gall,
    in_sem, round_sem, aux_tx, aux_rx, rx, srow, crow, ccol, ecol,
    so, sr, sot, srt, dd, ddt, bb, bbt, pp, ppt,
    hh, rim, rim_tx, gt_tx, gt_rx,
    eact, edsilu, cemb, pre0, pre1, act0, act1, msg, gm0, gm1, ga1, gp, gs_own, gs_rim, gd, gh,
    acc, g1, g0, ge, px1, px0, pxe, tx1, tx0, txe, gr, ag, gv, bcol, bdt, bpt, xs, swap_send, swap_recv,
    pair_send, pair_recv,
    a2a_send, a2a_recv, aux_send, aux_recv, rim_send, rim_recv, gt_send, gt_recv,
    rs_send, rs_recv, ag_send, ag_recv, own_sem,
):
    (cols, live, cweight, slot, static, bidx, esrc, edst, elive, eweight,
     enc_in, enc_out, src_proj, dst_proj, msg_proj, cot) = copies
    n_dev = n_grid * n_dom
    n_node = static.shape[0]
    n_edge = so.shape[0]
    n_col = cols.shape[0]
    n_bnd = bb.shape[0]
    rows_e = n_edge // LANES
    rows_c = n_col // LANES
    g = lax.axis_index("grid")
    o = lax.axis_index("dom")
    me = g * n_dom + o

    core = lax.rem(g, 2)
    z = g // 2
    n_z, n_y, n_x = n_grid // 2, n_dom // 4, 4
    y, x = o // n_x, lax.rem(o, n_x)
    chip = z * n_dom + o
    n_chip = n_dev // 2

    def others(fn, cores=(1, 0)):
        def some(i, skip):
            to_z = lax.rem(z + (n_z - 1 - i // n_y), n_z)
            to_y = lax.rem(y + (n_y - 1 - lax.rem(i, n_y)), n_y)
            for dx in (2, 1, 3, 0):
                to_o = to_y * n_x + lax.rem(x + dx, n_x)
                for dc in cores:
                    if not (skip and dx == 0 and dc == 0):
                        fn(to_z * 2 + (1 - core if dc else core), to_o)

        def body(i, carry):
            some(i, False)
            return carry
        lax.fori_loop(0, n_z * n_y - 1, body, 0)
        some(n_z * n_y - 1, True)

    def loop(n, fn):
        def body(k, carry):
            fn(k)
            return carry
        lax.fori_loop(0, n, body, 0)

    def load(i):
        return pltpu.make_async_copy(inputs[i], copies[i], in_sem.at[i])

    barrier = pltpu.get_barrier_semaphore()

    def column(fn):
        for k in range(1, n_grid):
            fn((lax.rem(g + k, n_grid), o))

    def greet(sem, to):
        pl.semaphore_signal(sem, inc=1, device_id=to, device_id_type=MESH)

    for k in range(1, n_dom):
        greet(barrier, (g, lax.rem(o + k, n_dom)))
    column(lambda to: greet(barrier, to))
    order = (0, 1, 2, 3, 6, 7, 8, 9, 5, 15, 14, 10, 11, 4, 12, 13)
    for i in order:
        load(i).start()
    for i in order[:4]:
        load(i).wait()

    lane = lax.broadcasted_iota(jnp.int32, (rows_c, LANES), 1)
    quarter = lax.rem(me, 4)
    slot_f = slot[...].astype(F32)
    scale_f = cweight[...] * live[...].astype(F32)
    for j in range(8):
        to_slot = lax.rem((quarter - j) * 16 + 2 * LANES, LANES)
        to_scale = lax.rem((quarter - j) * 16 + 64 + 2 * LANES, LANES)
        a = pltpu.roll(slot_f, to_slot, axis=1)
        b = pltpu.roll(scale_f, to_scale, axis=1)
        row = jnp.where(lane // 16 == quarter, a, jnp.where(lane // 16 == quarter + 4, b, 0.0))
        aux_tx[pl.ds(j, rows_c, stride=8), :] = row

    pl.semaphore_wait(barrier, n_dom + n_grid - 2)
    column(lambda to: greet(round_sem, to))
    pl.semaphore_wait(round_sem, n_grid - 1)

    def send_aux(to_g, to_o):
        d = to_g * n_dom + to_o
        pltpu.make_async_remote_copy(
            src_ref=aux_tx.at[d], dst_ref=aux_rx.at[me],
            send_sem=aux_send, recv_sem=aux_recv, device_id=(to_g, to_o), device_id_type=MESH,
        ).start()

    def send_cols(to_g, to_o):
        d = to_g * n_dom + to_o
        pltpu.make_async_remote_copy(
            src_ref=cols.at[pl.ds(pl.multiple_of(d * TILE, TILE), TILE), :],
            dst_ref=rx.at[pl.ds(pl.multiple_of(me * TILE, TILE), TILE), :],
            send_sem=a2a_send, recv_sem=a2a_recv.at[z], device_id=(to_g, to_o), device_id_type=MESH,
        ).start()

    others(send_aux)
    others(send_cols)
    for i in order[4:]:
        load(i).wait()
    mine = pl.ds(pl.multiple_of(me * TILE, TILE), TILE)
    rx[mine, :] = cols[mine, :]
    aux_rx[me] = aux_tx[me]

    here = (g > 0, g < n_grid - 1, o > 0, o < n_dom - 1)
    near = ((g - 1, o), (g + 1, o), (g, o - 1), (g, o + 1))
    flip = (1, 0, 3, 2)
    for r in range(4):
        @pl.when(jnp.logical_not(here[r]))
        def _():
            for l in range(2):
                rim[l, r] = jnp.zeros((n_bnd, 256), BF)
                gt_rx[l, flip[r]] = jnp.zeros((n_bnd, 256), BF)

    lane_i = lax.broadcasted_iota(jnp.int32, (LANES, LANES), 1)
    sub_i = lax.broadcasted_iota(jnp.int32, (LANES, LANES), 0)

    def across(row):
        full = jnp.broadcast_to(row, (LANES, LANES))
        return full, jnp.transpose(full)

    def build_edges(b):
        at = pl.ds(pl.multiple_of(b * LANES, LANES), LANES)
        full, down = across(edst[pl.ds(b, 1), :])
        for c in range(n_node // LANES):
            part = slice(c * LANES, (c + 1) * LANES)
            dd[at, part] = hot(down == lane_i + c * LANES)
            ddt[part, at] = hot(full == sub_i + c * LANES)
        for c in range(n_bnd // LANES):
            part = slice(c * LANES, (c + 1) * LANES)
            bdt[part, at] = hot(full == bcol[part, :])
        scale = eweight[pl.ds(b, 1), :] * elive[pl.ds(b, 1), :].astype(F32)
        ecol[at, :] = across(scale)[1]
        full, down = across(esrc[pl.ds(b, 1), :])
        for c in range(n_node // LANES):
            part = slice(c * LANES, (c + 1) * LANES)
            so[at, part] = hot(down == lane_i + c * LANES)
            sot[part, at] = hot(full == sub_i + c * LANES)
        for c in range(4 * n_bnd // LANES):
            part = slice(c * LANES, (c + 1) * LANES)
            sr[at, part] = hot(down == lane_i + (n_node + c * LANES))
            srt[part, at] = hot(full == sub_i + (n_node + c * LANES))

    def build_bound(b):
        at = pl.ds(pl.multiple_of(b * LANES, LANES), LANES)
        full, down = across(bidx[pl.ds(b, 1), :])
        for c in range(n_node // LANES):
            part = slice(c * LANES, (c + 1) * LANES)
            bb[at, part] = hot(down == lane_i + c * LANES)
            bbt[part, at] = hot(full == sub_i + c * LANES)
        bcol[at, :] = down

    loop(n_bnd // LANES, build_bound)
    loop(rows_e, build_edges)

    def chunk(c):
        return pl.ds(pl.multiple_of(c * CH, CH), CH)

    def node_chunk(c):
        return pl.ds(pl.multiple_of(c * CN, CN), CN)

    def back_last(c):
        at = chunk(c)
        rows = (mm(dd[at, :], cot[...]) * wide(ecol[at, :])).astype(BF)
        gm1[at, :] = rows
        ga1[at, :] = mt(rows, msg_proj[1])

    loop(n_edge // CH, back_last)

    got = pl.ds(0, (n_dev - 1) * TILE)
    cols_done = pltpu.make_async_remote_copy(
        src_ref=rx.at[got, :], dst_ref=rx.at[got, :], send_sem=a2a_send, recv_sem=a2a_recv.at[0],
        device_id=(g, o), device_id_type=MESH)
    got_aux = pl.ds(0, n_dev - 1)
    aux_done = pltpu.make_async_remote_copy(
        src_ref=aux_rx.at[got_aux], dst_ref=aux_rx.at[got_aux], send_sem=aux_send, recv_sem=aux_recv,
        device_id=(g, o), device_id_type=MESH)
    aux_done.wait_recv()
    parts = aux_rx[...].reshape(rows_c, 8, LANES)
    low = jnp.sum(parts[:, 0:4, :], axis=1)
    high = jnp.sum(parts[:, 4:8, :], axis=1)
    srow[...] = jnp.where(lane < 64, low, pltpu.roll(high, 64, axis=1))
    crow[...] = jnp.where(lane < 64, pltpu.roll(low, 64, axis=1), high)

    lane_f = lane_i.astype(F32)
    sub_f = sub_i.astype(F32)

    def build_pool(b):
        at = pl.ds(pl.multiple_of(b * LANES, LANES), LANES)
        full, down = across(srow[pl.ds(b, 1), :])
        for c in range(n_node // LANES):
            part = slice(c * LANES, (c + 1) * LANES)
            pp[at, part] = hot(down == lane_f + float(c * LANES))
            ppt[part, at] = hot(full == sub_f + float(c * LANES))
        for c in range(n_bnd // LANES):
            part = slice(c * LANES, (c + 1) * LANES)
            bpt[part, at] = hot(full == bcol[part, :].astype(F32))
        ccol[at, :] = across(crow[pl.ds(b, 1), :])[1]

    loop(rows_c, build_pool)

    def sigmoid(v):
        return 0.5 * jnp.tanh(0.5 * v) + 0.5

    plane = n_col // n_z

    def encode(to_z):
        at = pl.ds(pl.multiple_of(to_z * plane, plane), plane)
        v = mm(rx[at, :], enc_in[...])
        s = sigmoid(v)
        a = (v * s).astype(BF)
        eact[at, :] = a
        edsilu[at, :] = s * (1.0 + v * (1.0 - s))
        cemb[at, :] = (mm(a, enc_out[...]) * wide(ccol[at, :])).astype(BF)

    for dz in reversed(range(n_z)):
        from_z = lax.rem(z - dz + n_z, n_z)
        got = pl.ds(0, plane - (TILE if dz == 0 else 0))
        pltpu.make_async_remote_copy(
            src_ref=rx.at[got, :], dst_ref=rx.at[got, :], send_sem=a2a_send, recv_sem=a2a_recv.at[from_z],
            device_id=(g, o), device_id_type=MESH).wait_recv()
        encode(from_z)

    def pool(c):
        at = node_chunk(c)
        hh[0, at, :] = (static[at, :].astype(F32) + mm(ppt[at, :], cemb[...])).astype(BF)


    def fwd_copy(l, r):
        return pltpu.make_async_remote_copy(
            src_ref=rim_tx.at[l], dst_ref=rim.at[l, r], send_sem=rim_send.at[l, r],
            recv_sem=rim_recv.at[l, r], device_id=near[flip[r]], device_id_type=MESH)

    def back_copy(l, r):
        return pltpu.make_async_remote_copy(
            src_ref=gt_tx.at[l, r], dst_ref=gt_rx.at[l, r], send_sem=gt_send.at[l, r],
            recv_sem=gt_recv.at[l, r], device_id=near[r], device_id_type=MESH)

    def send_rims(l):
        if l == 0:
            rows = mm(bb[...], static[...]) + mm(bpt[...], cemb[...])
        else:
            rows = mm(bb[...], hh[0]) + mm(bdt[...], msg[...])
        rim_tx[l] = rows.astype(BF)
        for r in (2, 3, 0, 1):
            @pl.when(here[flip[r]])
            def _():
                fwd_copy(l, r).start()

    def wait_rims(l, blocks):
        for r in blocks:
            @pl.when(here[r])
            def _():
                fwd_copy(l, r).wait_recv()

    def layer_own(l, pre):
        def body(c):
            at = chunk(c)
            h = hh[l]
            xo = mm(so[at, :], h).astype(BF)
            xd = mm(dd[at, :], h).astype(BF)
            pre[at, :] = mm(xo, src_proj[l]) + mm(xd, dst_proj[l])
        loop(n_edge // CH, body)

    def layer_grid(l):
        def body(c):
            at = chunk(c)
            xs[at, :] = mm(sr[at, 0:2 * n_bnd], rim[l, 0:2].reshape(2 * n_bnd, 256)).astype(BF)
        loop(n_edge // CH, body)

    def layer_rest(l, pre, act):
        def body(c):
            at = chunk(c)
            xr = mm(sr[at, 2 * n_bnd:], rim[l, 2:4].reshape(2 * n_bnd, 256))
            xr = (xr + xs[at, :].astype(F32)).astype(BF)
            v = pre[at, :] + mm(xr, src_proj[l])
            s = sigmoid(v)
            a = (v * s).astype(BF)
            act[at, :] = a
            slope = s * (1.0 + v * (1.0 - s))
            if l == 0:
                pre[at, :] = slope
            else:
                gp[at, :] = (ga1[at, :] * slope).astype(BF)
            msg[at, :] = (mm(a, msg_proj[l]) * wide(ecol[at, :])).astype(BF)
        loop(n_edge // CH, body)

    def gather_messages(l):
        def body(c):
            at = node_chunk(c)
            rows = (hh[l, at, :].astype(F32) + mm(ddt[at, :], msg[...])).astype(BF)
            if l == 0:
                hh[1, at, :] = rows
            else:
                node_out[at, :] = rows
        loop(n_node // CN, body)

    send_rims(0)
    loop(n_node // CN, pool)
    layer_own(0, pre0)
    wait_rims(0, (0, 1))
    layer_grid(0)
    wait_rims(0, (2, 3))
    layer_rest(0, pre0, act0)
    send_rims(1)
    gather_messages(0)
    layer_own(1, pre1)
    wait_rims(1, (0, 1))
    layer_grid(1)
    wait_rims(1, (2, 3))
    layer_rest(1, pre1, act1)

    def back_rims(l):
        for r in (2, 3, 0, 1):
            rows = mm(srt[r * n_bnd:(r + 1) * n_bnd, :], gp[...]).astype(BF)
            gs_rim[r] = rows
            gt_tx[l, r] = mt(rows, src_proj[l]).astype(BF)

            @pl.when(here[r])
            def _():
                back_copy(l, r).start()

    def back_own(l):
        def body(c):
            at = node_chunk(c)
            s_rows = mm(sot[at, :], gp[...]).astype(BF)
            d_rows = mm(ddt[at, :], gp[...]).astype(BF)
            gs_own[at, :] = s_rows
            gd[at, :] = d_rows
            before = cot[at, :].astype(F32) if l == 1 else gh[at, :]
            gh[at, :] = before + mt(s_rows, src_proj[l]) + mt(d_rows, dst_proj[l])
        loop(n_node // CN, body)

    def halves(out, first, value):
        rows = slice(first, first + value.shape[0])
        out[0, rows, :] = value[:, 0:LANES]
        out[1, rows, :] = value[:, LANES:]

    def layer_weights(l, act, gm, out):
        total = tm(hh[l], gs_own[...])
        for r in range(4):
            total = total + tm(rim[l, r], gs_rim[r])
        halves(out, 0, total)
        halves(out, 256, tm(hh[l], gd[...]))
        acc[...] = jnp.zeros_like(acc)

        def body(c):
            at = chunk(c)
            acc[...] += tm(act[at, :], gm[at, :])
        loop(n_edge // CH, body)
        halves(out, 512, acc[...])

    def add_rims(l):
        for r in range(4):
            @pl.when(here[flip[r]])
            def _():
                back_copy(l, r).wait_recv()

        def body(c):
            at = node_chunk(c)
            total = gh[at, :]
            for r in range(4):
                total = total + mm(bbt[at, :], gt_rx[l, r])
            gh[at, :] = total
        loop(n_node // CN, body)

    rounds = ((48, 0, 0), (48, 48, 48), (24, 32, 96))
    parts_of = ((g1, px1, tx1), (g0, px0, tx0), (ge, pxe, txe))

    def tile_of(k, q):
        return lax.rem(q - rounds[k][1] + n_chip, n_chip)

    def pair_copy(k):
        mine, theirs, _ = parts_of[k]
        return pltpu.make_async_remote_copy(
            src_ref=mine.at[1 - core], dst_ref=theirs, send_sem=pair_send.at[k],
            recv_sem=pair_recv.at[k], device_id=(g + 1 - 2 * core, o), device_id_type=MESH)

    def rows_of(t):
        return pl.ds(pl.multiple_of(t * TILE, TILE), TILE)

    def scatter_start(k):
        count = rounds[k][0]
        mine, theirs, out = parts_of[k]
        pair_copy(k).wait_recv()

        def add(c):
            at = pl.ds(pl.multiple_of(c * LANES, LANES), LANES)
            out[at, :] = (mine[core, at, :] + theirs[at, :]).astype(BF)
        loop(out.shape[0] // LANES, add)

        def one(to_g, to_o):
            t = tile_of(k, (to_g // 2) * n_dom + to_o)

            @pl.when(t < count)
            def _():
                pltpu.make_async_remote_copy(
                    src_ref=out.at[rows_of(t), :], dst_ref=gr.at[k, chip], send_sem=rs_send.at[k],
                    recv_sem=rs_recv.at[k], device_id=(to_g, to_o), device_id_type=MESH).start()
        others(one, cores=(0,))

        @pl.when(tile_of(k, chip) < count)
        def _():
            gr[k, chip] = out[rows_of(tile_of(k, chip)), :]

    def span_wait(ref, n, sem, what):
        at = pl.ds(0, n)
        copy = pltpu.make_async_remote_copy(
            src_ref=ref.at[at], dst_ref=ref.at[at], send_sem=sem, recv_sem=sem,
            device_id=(g, o), device_id_type=MESH)
        if what == "recv":
            copy.wait_recv()
        else:
            copy.wait_send()

    def place(k):
        return gv.at[core, rounds[k][2] + tile_of(k, chip)]

    def gather_start(k):
        @pl.when(tile_of(k, chip) < rounds[k][0])
        def _():
            span_wait(gr.at[k], n_chip - 1, rs_recv.at[k], "recv")

            def body(s, totals):
                return tuple(
                    totals[i] + gr[k, s * 8 + i].astype(F32) + gr[k, s * 8 + i + 4].astype(F32)
                    for i in range(4))
            zero = jnp.zeros((TILE, LANES), F32)
            totals = lax.fori_loop(0, n_chip // 8, body, (zero,) * 4)
            total = ((totals[0] + totals[1]) + (totals[2] + totals[3])).astype(BF)
            ag[k] = total
            gv[core, rounds[k][2] + tile_of(k, chip)] = total

            def one(to_g, to_o):
                pltpu.make_async_remote_copy(
                    src_ref=ag.at[k], dst_ref=place(k), send_sem=ag_send.at[k],
                    recv_sem=ag_recv.at[k], device_id=(to_g, to_o), device_id_type=MESH).start()
            others(one, cores=(0,))

    def swap_copy(k):
        part = gv.at[core, pl.ds(rounds[k][2], rounds[k][0])]
        return pltpu.make_async_remote_copy(
            src_ref=part, dst_ref=part, send_sem=swap_send.at[k], recv_sem=swap_recv.at[k],
            device_id=(g + 1 - 2 * core, o), device_id_type=MESH)

    def swap_start(k):
        count = rounds[k][0]

        @pl.when(tile_of(k, chip) < count)
        def _():
            span_wait(gr.at[k], count - 1, ag_recv.at[k], "recv")

        @pl.when(tile_of(k, chip) >= count)
        def _():
            span_wait(gr.at[k], count, ag_recv.at[k], "recv")
        swap_copy(k).start()

    def out_copy(k):
        part = pl.ds(rounds[k][2], rounds[k][0])
        return pltpu.make_async_copy(gv.at[:, part], gall.at[:, part], own_sem.at[k])

    def out_start(k):
        swap_copy(k).wait_recv()
        out_copy(k).start()

    def finish(k):
        count = rounds[k][0]
        pair_copy(k).wait_send()
        swap_copy(k).wait_send()

        @pl.when(tile_of(k, chip) < count)
        def _():
            span_wait(gr.at[k], count - 1, rs_send.at[k], "send")
            span_wait(gr.at[k], n_chip - 1, ag_send.at[k], "send")

        @pl.when(tile_of(k, chip) >= count)
        def _():
            span_wait(gr.at[k], count, rs_send.at[k], "send")
        out_copy(k).wait()

    back_rims(1)
    back_own(1)
    layer_weights(1, act1, gm1, g1)
    pair_copy(0).start()
    gather_messages(1)
    scatter_start(0)
    add_rims(1)

    def back_first(c):
        at = chunk(c)
        rows = (mm(dd[at, :], gh[...].astype(BF)) * wide(ecol[at, :])).astype(BF)
        gm0[at, :] = rows
        gp[at, :] = (mt(rows, msg_proj[0]) * pre0[at, :]).astype(BF)

    loop(n_edge // CH, back_first)
    back_rims(0)
    gather_start(0)
    back_own(0)
    layer_weights(0, act0, gm0, g0)
    pair_copy(1).start()
    scatter_start(1)
    add_rims(0)

    acc[...] = jnp.zeros_like(acc)

    def encode_out(c):
        at = chunk(c)
        rows = (mm(pp[at, :], gh[...].astype(BF)) * wide(ccol[at, :])).astype(BF)
        acc[...] += tm(eact[at, :], rows)
        cemb[at, :] = (mt(rows, enc_out[...]) * edsilu[at, :]).astype(BF)

    loop(n_col // CH, encode_out)
    halves(ge, 0, acc[...])
    acc[...] = jnp.zeros_like(acc)

    def encode_in(c):
        at = chunk(c)
        acc[0:128, :] += tm(rx[at, :], cemb[at, :])

    loop(n_col // CH, encode_in)
    halves(ge, 256, acc[0:128, :])
    pair_copy(2).start()
    scatter_start(2)
    gather_start(1)
    swap_start(0)
    out_start(0)
    gather_start(2)
    swap_start(1)
    out_start(1)
    swap_start(2)
    out_start(2)

    cols_done.wait_send()
    aux_done.wait_send()
    for l in range(2):
        for r in range(4):
            @pl.when(here[flip[r]])
            def _():
                fwd_copy(l, r).wait_send()

            @pl.when(here[r])
            def _():
                back_copy(l, r).wait_send()
    for k in range(3):
        finish(k)


def finish_kernel(gall, node_in, enc_in_g, enc_out_g, src_g, dst_g, msg_g, node_out,
                  tiles, mats, nodes, in_sem, out_sem):
    jobs = []
    for layer, first in ((1, 0), (0, 48)):
        for m, ref in enumerate((src_g, dst_g, msg_g)):
            jobs.append((first + 16 * m, 16, ref.at[layer]))
    jobs.append((96, 16, enc_out_g))
    jobs.append((112, 8, enc_in_g))
    n = len(jobs)

    def fetch(i):
        at = pl.ds(jobs[i][0], jobs[i][1])
        return pltpu.make_async_copy(gall.at[:, at], tiles.at[:, at], in_sem.at[i])

    def put(i):
        return pltpu.make_async_copy(mats.at[i, pl.ds(0, jobs[i][1] * TILE)], jobs[i][2], out_sem.at[i])

    node_fetch = pltpu.make_async_copy(node_in, nodes, in_sem.at[n])
    node_put = pltpu.make_async_copy(nodes, node_out, out_sem.at[n])
    for i in range(n):
        fetch(i).start()
    node_fetch.start()
    for i in range(n):
        fetch(i).wait()
        first, count, _ = jobs[i]
        for half in range(2):
            block = tiles[half, first:first + count].astype(F32).reshape(count * TILE, LANES)
            mats[i, 0:count * TILE, half * LANES:(half + 1) * LANES] = block
        put(i).start()
    node_fetch.wait()
    node_put.start()
    for i in range(n):
        put(i).wait()
    node_put.wait()


def per_device(n_grid, n_dom, columns, column_live, col_weight, col_slot, node_static, boundary_idx,
               edge_src, edge_dst, edge_live, edge_weight, enc_in, enc_out, src_proj, dst_proj, msg_proj,
               node_cotangent):
    n_dev = n_grid * n_dom
    n_col = columns.shape[0]
    n_edge = edge_src.shape[0]
    n_node, width = node_static.shape
    n_bnd = boundary_idx.shape[0]
    rows = lambda x: x.reshape(-1, LANES)
    vm = lambda *shape: pltpu.VMEM(shape, BF)
    vf = lambda *shape: pltpu.VMEM(shape, F32)
    dma = pltpu.SemaphoreType.DMA
    args = (columns, rows(column_live), rows(col_weight), rows(col_slot), node_static, rows(boundary_idx),
            rows(edge_src), rows(edge_dst), rows(edge_live), rows(edge_weight), enc_in, enc_out, src_proj,
            dst_proj, msg_proj, node_cotangent)
    scratch = [pltpu.VMEM(a.shape, a.dtype) for a in args] + [
        dma((len(args),)), pltpu.SemaphoreType.REGULAR,
        vf(n_dev, LANES), vf(n_dev, LANES), vm(n_col, columns.shape[1]), vf(n_col // LANES, LANES),
        vf(n_col // LANES, LANES), vf(n_col, LANES), vf(n_edge, LANES),
        vm(n_edge, n_node), vm(n_edge, 4 * n_bnd), vm(n_node, n_edge), vm(4 * n_bnd, n_edge),
        vm(n_edge, n_node), vm(n_node, n_edge), vm(n_bnd, n_node), vm(n_node, n_bnd),
        vm(n_col, n_node), vm(n_node, n_col),
        vm(2, n_node, width), vm(2, 4, n_bnd, width), vm(2, n_bnd, width), vm(2, 4, n_bnd, width),
        vm(2, 4, n_bnd, width),
        vm(n_col, width), vf(n_col, width), vm(n_col, width), vf(n_edge, width), vf(n_edge, width),
        vm(n_edge, width), vm(n_edge, width), vm(n_edge, width), vm(n_edge, width), vm(n_edge, width),
        vf(n_edge, width), vm(n_edge, width), vm(n_node, width), vm(4, n_bnd, width), vm(n_node, width),
        vf(n_node, width),
        vf(width, width), vf(2, 768, LANES), vf(2, 768, LANES), vf(2, 384, LANES),
        vf(768, LANES), vf(768, LANES), vf(384, LANES), vm(768, LANES), vm(768, LANES), vm(384, LANES),
        vm(3, n_dev // 2, TILE, LANES), vm(3, TILE, LANES), vm(2, 120, TILE, LANES),
        pltpu.VMEM((n_bnd, LANES), jnp.int32), vm(n_bnd, n_edge), vm(n_bnd, n_col), vm(n_edge, width),
        dma((3,)), dma((3,)), dma((3,)), dma((3,)),
        dma(()), dma((n_grid // 2,)), dma(()), dma(()), dma((2, 4)), dma((2, 4)), dma((2, 4)), dma((2, 4)),
        dma((3,)), dma((3,)), dma((3,)), dma((3,)), dma((3,)),
    ]
    in_vmem = pl.BlockSpec(memory_space=pltpu.VMEM)
    in_hbm = pl.BlockSpec(memory_space=pl.ANY)
    node_out, gall = pl.pallas_call(
        functools.partial(step_kernel, n_grid, n_dom, len(args)),
        out_shape=(jax.ShapeDtypeStruct((n_node, width), BF), jax.ShapeDtypeStruct((2, 120, TILE, LANES), BF)),
        in_specs=[pl.BlockSpec(memory_space=pl.ANY)] * len(args),
        out_specs=(in_vmem, pl.BlockSpec(memory_space=pl.ANY)),
        scratch_shapes=scratch,
        compiler_params=pltpu.CompilerParams(
            collective_id=0, has_side_effects=True, vmem_limit_bytes=62 * 1024 * 1024),
    )(*args)
    mat = jax.ShapeDtypeStruct((width, width), F32)
    pair = jax.ShapeDtypeStruct((2, width, width), F32)
    enc_in_g, enc_out_g, src_g, dst_g, msg_g, node_final = pl.pallas_call(
        finish_kernel,
        out_shape=(jax.ShapeDtypeStruct(enc_in.shape, F32), mat, pair, pair, pair,
                   jax.ShapeDtypeStruct((n_node, width), BF)),
        in_specs=[in_hbm] * 2,
        out_specs=(in_hbm,) * 6,
        scratch_shapes=[vm(2, 120, TILE, LANES), vf(8, width, width), vm(n_node, width), dma((9,)), dma((9,))],
    )(gall, node_out)
    return (node_final, enc_in_g, enc_out_g, src_g, dst_g, msg_g)


def solution(mesh):
    n_grid, n_dom = mesh.shape["grid"], mesh.shape["dom"]
    both = P(("grid", "dom"))
    rows = P(("grid", "dom"), None)
    placed = (rows, both, both, both, rows, both, both, both, both, both, P(), P(), P(), P(), P(), rows)
    return jax.shard_map(
        functools.partial(per_device, n_grid, n_dom),
        mesh=mesh,
        in_specs=placed,
        out_specs=(rows, P(), P(), P(), P(), P()),
        check_vma=False,
    )
```

```python
import functools

import jax
import jax.numpy as jnp
from jax import lax
from jax.experimental import pallas as pl
from jax.experimental.pallas import tpu as pltpu
from jax.sharding import PartitionSpec as P

MESH = pl.DeviceIdType.MESH
BF = jnp.bfloat16
F32 = jnp.float32
CH = 1024
CN = 512
LANES = 128
TILE = 16


def mm(a, b):
    return lax.dot_general(a, b, (((1,), (0,)), ((), ())), preferred_element_type=F32)


def mt(a, b):
    return lax.dot_general(a, b, (((1,), (1,)), ((), ())), preferred_element_type=F32)


def tm(a, b):
    return lax.dot_general(a, b, (((0,), (0,)), ((), ())), preferred_element_type=F32)


def wide(x):
    return jnp.concatenate([x, x], axis=1)


def hot(equal):
    return jnp.where(equal, 1.0, 0.0).astype(BF)


def step_kernel(
    n_grid, n_dom,
    n_in, *refs,
):
    inputs = refs[:n_in]
    outs = refs[n_in:n_in + 3]
    copies = refs[n_in + 3:2 * n_in + 3]
    step_body(n_grid, n_dom, inputs, copies, *outs, *refs[2 * n_in + 3:])


def step_body(
    n_grid, n_dom, inputs, copies, node_out, gall, gall_enc,
    in_sem, round_sem, aux_tx, aux_rx, rx, srow, crow, ccol, ecol,
    so, sr, sot, srt, dd, ddt, bb, bbt, pp, ppt,
    hh, rim, rim_tx, gt_tx, gt_rx,
    eact, edsilu, cemb, pre0, pre1, act0, act1, msg, gm0, gm1, ga1, gp, gs_own, gs_rim, gd, gh,
    acc, g1, g0, ge, px1, px0, pxe, tx1, tx0, txe, gr, gre, ag, age, gv, bcol, bdt, bpt, xs, swap_send, swap_recv,
    pair_send, pair_recv,
    a2a_send, a2a_recv, aux_send, aux_recv, rim_send, rim_recv, gt_send, gt_recv,
    rs_send, rs_recv, ag_send, ag_recv, own_sem,
):
    (cols, live, cweight, slot, static, bidx, esrc, edst, elive, eweight,
     enc_in, enc_out, src_proj, dst_proj, msg_proj, cot) = copies
    n_dev = n_grid * n_dom
    n_node = static.shape[0]
    n_edge = so.shape[0]
    n_col = cols.shape[0]
    n_bnd = bb.shape[0]
    rows_e = n_edge // LANES
    rows_c = n_col // LANES
    g = lax.axis_index("grid")
    o = lax.axis_index("dom")
    me = g * n_dom + o

    core = lax.rem(g, 2)
    z = g // 2
    n_z, n_y, n_x = n_grid // 2, n_dom // 4, 4
    y, x = o // n_x, lax.rem(o, n_x)
    chip = z * n_dom + o
    n_chip = n_dev // 2

    def others(fn, cores=(1, 0)):
        def some(i, skip):
            to_z = lax.rem(z + (n_z - 1 - i // n_y), n_z)
            to_y = lax.rem(y + (n_y - 1 - lax.rem(i, n_y)), n_y)
            for dx in (2, 1, 3, 0):
                to_o = to_y * n_x + lax.rem(x + dx, n_x)
                for dc in cores:
                    if not (skip and dx == 0 and dc == 0):
                        fn(to_z * 2 + (1 - core if dc else core), to_o)

        def body(i, carry):
            some(i, False)
            return carry
        lax.fori_loop(0, n_z * n_y - 1, body, 0)
        some(n_z * n_y - 1, True)

    def loop(n, fn):
        def body(k, carry):
            fn(k)
            return carry
        lax.fori_loop(0, n, body, 0)

    def load(i):
        return pltpu.make_async_copy(inputs[i], copies[i], in_sem.at[i])

    barrier = pltpu.get_barrier_semaphore()

    def column(fn):
        for k in range(1, n_grid):
            fn((lax.rem(g + k, n_grid), o))

    def greet(sem, to):
        pl.semaphore_signal(sem, inc=1, device_id=to, device_id_type=MESH)

    for k in range(1, n_dom):
        greet(barrier, (g, lax.rem(o + k, n_dom)))
    column(lambda to: greet(barrier, to))
    order = (0, 1, 2, 3, 6, 7, 8, 9, 5, 15, 14, 10, 11, 4, 12, 13)
    for i in order:
        load(i).start()
    for i in order[:4]:
        load(i).wait()

    lane = lax.broadcasted_iota(jnp.int32, (rows_c, LANES), 1)
    quarter = lax.rem(me, 4)
    slot_f = slot[...].astype(F32)
    scale_f = cweight[...] * live[...].astype(F32)
    for j in range(8):
        to_slot = lax.rem((quarter - j) * 16 + 2 * LANES, LANES)
        to_scale = lax.rem((quarter - j) * 16 + 64 + 2 * LANES, LANES)
        a = pltpu.roll(slot_f, to_slot, axis=1)
        b = pltpu.roll(scale_f, to_scale, axis=1)
        row = jnp.where(lane // 16 == quarter, a, jnp.where(lane // 16 == quarter + 4, b, 0.0))
        aux_tx[pl.ds(j, rows_c, stride=8), :] = row

    pl.semaphore_wait(barrier, n_dom + n_grid - 2)
    column(lambda to: greet(round_sem, to))
    pl.semaphore_wait(round_sem, n_grid - 1)

    def send_aux(to_g, to_o):
        d = to_g * n_dom + to_o
        pltpu.make_async_remote_copy(
            src_ref=aux_tx.at[d], dst_ref=aux_rx.at[me],
            send_sem=aux_send, recv_sem=aux_recv, device_id=(to_g, to_o), device_id_type=MESH,
        ).start()

    def send_cols(to_g, to_o):
        d = to_g * n_dom + to_o
        pltpu.make_async_remote_copy(
            src_ref=cols.at[pl.ds(pl.multiple_of(d * TILE, TILE), TILE), :],
            dst_ref=rx.at[pl.ds(pl.multiple_of(me * TILE, TILE), TILE), :],
            send_sem=a2a_send, recv_sem=a2a_recv.at[z], device_id=(to_g, to_o), device_id_type=MESH,
        ).start()

    others(send_aux)
    others(send_cols)
    for i in order[4:]:
        load(i).wait()
    mine = pl.ds(pl.multiple_of(me * TILE, TILE), TILE)
    rx[mine, :] = cols[mine, :]
    aux_rx[me] = aux_tx[me]

    here = (g > 0, g < n_grid - 1, o > 0, o < n_dom - 1)
    near = ((g - 1, o), (g + 1, o), (g, o - 1), (g, o + 1))
    flip = (1, 0, 3, 2)
    for r in range(4):
        @pl.when(jnp.logical_not(here[r]))
        def _():
            for l in range(2):
                rim[l, r] = jnp.zeros((n_bnd, 256), BF)
                gt_rx[l, flip[r]] = jnp.zeros((n_bnd, 256), BF)

    lane_i = lax.broadcasted_iota(jnp.int32, (LANES, LANES), 1)
    sub_i = lax.broadcasted_iota(jnp.int32, (LANES, LANES), 0)

    def across(row):
        full = jnp.broadcast_to(row, (LANES, LANES))
        return full, jnp.transpose(full)

    def build_edges(b):
        at = pl.ds(pl.multiple_of(b * LANES, LANES), LANES)
        full, down = across(edst[pl.ds(b, 1), :])
        for c in range(n_node // LANES):
            part = slice(c * LANES, (c + 1) * LANES)
            dd[at, part] = hot(down == lane_i + c * LANES)
            ddt[part, at] = hot(full == sub_i + c * LANES)
        for c in range(n_bnd // LANES):
            part = slice(c * LANES, (c + 1) * LANES)
            bdt[part, at] = hot(full == bcol[part, :])
        scale = eweight[pl.ds(b, 1), :] * elive[pl.ds(b, 1), :].astype(F32)
        ecol[at, :] = across(scale)[1]
        full, down = across(esrc[pl.ds(b, 1), :])
        for c in range(n_node // LANES):
            part = slice(c * LANES, (c + 1) * LANES)
            so[at, part] = hot(down == lane_i + c * LANES)
            sot[part, at] = hot(full == sub_i + c * LANES)
        for c in range(4 * n_bnd // LANES):
            part = slice(c * LANES, (c + 1) * LANES)
            sr[at, part] = hot(down == lane_i + (n_node + c * LANES))
            srt[part, at] = hot(full == sub_i + (n_node + c * LANES))

    def build_bound(b):
        at = pl.ds(pl.multiple_of(b * LANES, LANES), LANES)
        full, down = across(bidx[pl.ds(b, 1), :])
        for c in range(n_node // LANES):
            part = slice(c * LANES, (c + 1) * LANES)
            bb[at, part] = hot(down == lane_i + c * LANES)
            bbt[part, at] = hot(full == sub_i + c * LANES)
        bcol[at, :] = down

    loop(n_bnd // LANES, build_bound)
    loop(rows_e, build_edges)

    def chunk(c):
        return pl.ds(pl.multiple_of(c * CH, CH), CH)

    def node_chunk(c):
        return pl.ds(pl.multiple_of(c * CN, CN), CN)

    def back_last(c):
        at = chunk(c)
        rows = (mm(dd[at, :], cot[...]) * wide(ecol[at, :])).astype(BF)
        gm1[at, :] = rows
        ga1[at, :] = mt(rows, msg_proj[1])

    loop(n_edge // CH, back_last)

    got = pl.ds(0, (n_dev - 1) * TILE)
    cols_done = pltpu.make_async_remote_copy(
        src_ref=rx.at[got, :], dst_ref=rx.at[got, :], send_sem=a2a_send, recv_sem=a2a_recv.at[0],
        device_id=(g, o), device_id_type=MESH)
    got_aux = pl.ds(0, n_dev - 1)
    aux_done = pltpu.make_async_remote_copy(
        src_ref=aux_rx.at[got_aux], dst_ref=aux_rx.at[got_aux], send_sem=aux_send, recv_sem=aux_recv,
        device_id=(g, o), device_id_type=MESH)
    aux_done.wait_recv()
    parts = aux_rx[...].reshape(rows_c, 8, LANES)
    low = jnp.sum(parts[:, 0:4, :], axis=1)
    high = jnp.sum(parts[:, 4:8, :], axis=1)
    srow[...] = jnp.where(lane < 64, low, pltpu.roll(high, 64, axis=1))
    crow[...] = jnp.where(lane < 64, pltpu.roll(low, 64, axis=1), high)

    lane_f = lane_i.astype(F32)
    sub_f = sub_i.astype(F32)

    def build_pool(b):
        at = pl.ds(pl.multiple_of(b * LANES, LANES), LANES)
        full, down = across(srow[pl.ds(b, 1), :])
        for c in range(n_node // LANES):
            part = slice(c * LANES, (c + 1) * LANES)
            pp[at, part] = hot(down == lane_f + float(c * LANES))
            ppt[part, at] = hot(full == sub_f + float(c * LANES))
        for c in range(n_bnd // LANES):
            part = slice(c * LANES, (c + 1) * LANES)
            bpt[part, at] = hot(full == bcol[part, :].astype(F32))
        ccol[at, :] = across(crow[pl.ds(b, 1), :])[1]

    loop(rows_c, build_pool)

    def sigmoid(v):
        return 0.5 * jnp.tanh(0.5 * v) + 0.5

    plane = n_col // n_z

    def encode(to_z):
        at = pl.ds(pl.multiple_of(to_z * plane, plane), plane)
        v = mm(rx[at, :], enc_in[...])
        s = sigmoid(v)
        a = (v * s).astype(BF)
        eact[at, :] = a
        edsilu[at, :] = s * (1.0 + v * (1.0 - s))
        cemb[at, :] = (mm(a, enc_out[...]) * wide(ccol[at, :])).astype(BF)

    for dz in reversed(range(n_z)):
        from_z = lax.rem(z - dz + n_z, n_z)
        got = pl.ds(0, plane - (TILE if dz == 0 else 0))
        pltpu.make_async_remote_copy(
            src_ref=rx.at[got, :], dst_ref=rx.at[got, :], send_sem=a2a_send, recv_sem=a2a_recv.at[from_z],
            device_id=(g, o), device_id_type=MESH).wait_recv()
        encode(from_z)

    def pool(c):
        at = node_chunk(c)
        hh[0, at, :] = (static[at, :].astype(F32) + mm(ppt[at, :], cemb[...])).astype(BF)


    def fwd_copy(l, r):
        return pltpu.make_async_remote_copy(
            src_ref=rim_tx.at[l], dst_ref=rim.at[l, r], send_sem=rim_send.at[l, r],
            recv_sem=rim_recv.at[l, r], device_id=near[flip[r]], device_id_type=MESH)

    def back_copy(l, r):
        return pltpu.make_async_remote_copy(
            src_ref=gt_tx.at[l, r], dst_ref=gt_rx.at[l, r], send_sem=gt_send.at[l, r],
            recv_sem=gt_recv.at[l, r], device_id=near[r], device_id_type=MESH)

    def send_rims(l):
        if l == 0:
            rows = mm(bb[...], static[...]) + mm(bpt[...], cemb[...])
        else:
            rows = mm(bb[...], hh[0]) + mm(bdt[...], msg[...])
        rim_tx[l] = rows.astype(BF)
        for r in (2, 3, 0, 1):
            @pl.when(here[flip[r]])
            def _():
                fwd_copy(l, r).start()

    def wait_rims(l, blocks):
        for r in blocks:
            @pl.when(here[r])
            def _():
                fwd_copy(l, r).wait_recv()

    def layer_own(l, pre):
        def body(c):
            at = chunk(c)
            h = hh[l]
            xo = mm(so[at, :], h).astype(BF)
            xd = mm(dd[at, :], h).astype(BF)
            pre[at, :] = mm(xo, src_proj[l]) + mm(xd, dst_proj[l])
        loop(n_edge // CH, body)

    def layer_grid(l):
        def body(c):
            at = chunk(c)
            xs[at, :] = mm(sr[at, 0:2 * n_bnd], rim[l, 0:2].reshape(2 * n_bnd, 256)).astype(BF)
        loop(n_edge // CH, body)

    def layer_rest(l, pre, act):
        def body(c):
            at = chunk(c)
            xr = mm(sr[at, 2 * n_bnd:], rim[l, 2:4].reshape(2 * n_bnd, 256))
            xr = (xr + xs[at, :].astype(F32)).astype(BF)
            v = pre[at, :] + mm(xr, src_proj[l])
            s = sigmoid(v)
            a = (v * s).astype(BF)
            act[at, :] = a
            if l == 0:
                pre[at, :] = v
                msg[at, :] = (mm(a, msg_proj[l]) * wide(ecol[at, :])).astype(BF)
            else:
                gp[at, :] = (ga1[at, :] * (s * (1.0 + v * (1.0 - s)))).astype(BF)
        loop(n_edge // CH, body)

    def slopes(c):
        at = chunk(c)
        v = pre0[at, :]
        s = sigmoid(v)
        pre0[at, :] = s * (1.0 + v * (1.0 - s))

    def last_messages(c):
        at = chunk(c)
        msg[at, :] = (mm(act1[at, :], msg_proj[1]) * wide(ecol[at, :])).astype(BF)

    def gather_messages(l):
        def body(c):
            at = node_chunk(c)
            rows = (hh[l, at, :].astype(F32) + mm(ddt[at, :], msg[...])).astype(BF)
            if l == 0:
                hh[1, at, :] = rows
            else:
                node_out[at, :] = rows
        loop(n_node // CN, body)

    send_rims(0)
    loop(n_node // CN, pool)
    layer_own(0, pre0)
    wait_rims(0, (0, 1))
    layer_grid(0)
    wait_rims(0, (2, 3))
    layer_rest(0, pre0, act0)
    send_rims(1)
    gather_messages(0)
    layer_own(1, pre1)
    wait_rims(1, (0, 1))
    layer_grid(1)
    wait_rims(1, (2, 3))
    layer_rest(1, pre1, act1)

    def back_rims(l):
        for r in (2, 3, 0, 1):
            rows = mm(srt[r * n_bnd:(r + 1) * n_bnd, :], gp[...]).astype(BF)
            gs_rim[r] = rows
            gt_tx[l, r] = mt(rows, src_proj[l]).astype(BF)

            @pl.when(here[r])
            def _():
                back_copy(l, r).start()

    def back_own(l):
        def body(c):
            at = node_chunk(c)
            s_rows = mm(sot[at, :], gp[...]).astype(BF)
            d_rows = mm(ddt[at, :], gp[...]).astype(BF)
            gs_own[at, :] = s_rows
            gd[at, :] = d_rows
            before = cot[at, :].astype(F32) if l == 1 else gh[at, :]
            gh[at, :] = before + mt(s_rows, src_proj[l]) + mt(d_rows, dst_proj[l])
        loop(n_node // CN, body)

    def halves(out, first, value):
        rows = slice(first, first + value.shape[0])
        out[0, rows, :] = value[:, 0:LANES]
        out[1, rows, :] = value[:, LANES:]

    def layer_weights(l, act, gm, out):
        total = tm(hh[l], gs_own[...])
        for r in range(4):
            total = total + tm(rim[l, r], gs_rim[r])
        halves(out, 0, total)
        halves(out, 256, tm(hh[l], gd[...]))
        acc[...] = jnp.zeros_like(acc)

        def body(c):
            at = chunk(c)
            acc[...] += tm(act[at, :], gm[at, :])
        loop(n_edge // CH, body)
        halves(out, 512, acc[...])

    def add_rims(l):
        for r in range(4):
            @pl.when(here[flip[r]])
            def _():
                back_copy(l, r).wait_recv()

        def body(c):
            at = node_chunk(c)
            total = gh[at, :]
            for r in range(4):
                total = total + mm(bbt[at, :], gt_rx[l, r])
            gh[at, :] = total
        loop(n_node // CN, body)

    rounds = ((48, 0, 0), (48, 48, 48), (48, 16, 0))
    parts_of = ((g1, px1, tx1), (g0, px0, tx0), (ge, pxe, txe))

    def tile_of(k, q):
        return lax.rem(q - rounds[k][1] + n_chip, n_chip)

    def pair_copy(k):
        mine, theirs, _ = parts_of[k]
        return pltpu.make_async_remote_copy(
            src_ref=mine.at[1 - core], dst_ref=theirs, send_sem=pair_send.at[k],
            recv_sem=pair_recv.at[k], device_id=(g + 1 - 2 * core, o), device_id_type=MESH)

    def rows_of(t):
        return pl.ds(pl.multiple_of(t * TILE, TILE), TILE)

    def held(k):
        return gre if k == 2 else gr.at[k]

    def scatter_start(k):
        def tile(ref, t):
            return ref.at[t] if k == 2 else ref.at[rows_of(t), :]

        count = rounds[k][0]
        mine, theirs, out = parts_of[k]
        pair_copy(k).wait_recv()

        def add(c):
            at = pl.ds(pl.multiple_of(c * LANES, LANES), LANES)
            total = mine[core, at, :] + theirs[at, :]
            if k < 2:
                out[at, :] = total.astype(BF)
            else:
                out[pl.ds(c * 16, 16)] = total.reshape(16, 8, LANES).astype(BF)
        loop(theirs.shape[0] // LANES, add)

        def one(to_g, to_o):
            t = tile_of(k, (to_g // 2) * n_dom + to_o)

            @pl.when(t < count)
            def _():
                pltpu.make_async_remote_copy(
                    src_ref=tile(out, t), dst_ref=held(k).at[chip], send_sem=rs_send.at[k],
                    recv_sem=rs_recv.at[k], device_id=(to_g, to_o), device_id_type=MESH).start()
        others(one, cores=(0,))

        @pl.when(tile_of(k, chip) < count)
        def _():
            held(k)[chip] = tile(out, tile_of(k, chip))[...]

    def span_wait(ref, n, sem, what):
        at = pl.ds(0, n)
        copy = pltpu.make_async_remote_copy(
            src_ref=ref.at[at], dst_ref=ref.at[at], send_sem=sem, recv_sem=sem,
            device_id=(g, o), device_id_type=MESH)
        if what == "recv":
            copy.wait_recv()
        else:
            copy.wait_send()

    def place(k):
        if k == 2:
            return gall_enc.at[core, tile_of(k, chip)]
        return gv.at[core, rounds[k][2] + tile_of(k, chip)]

    def own_copy():
        return pltpu.make_async_copy(age, place(2), own_sem.at[2])

    def gather_start(k):
        @pl.when(tile_of(k, chip) < rounds[k][0])
        def _():
            span_wait(held(k), n_chip - 1, rs_recv.at[k], "recv")

            def body(s, totals):
                return tuple(
                    totals[i] + held(k)[s * 8 + i].astype(F32) + held(k)[s * 8 + i + 4].astype(F32)
                    for i in range(4))
            zero = jnp.zeros((8 if k == 2 else TILE, LANES), F32)
            totals = lax.fori_loop(0, n_chip // 8, body, (zero,) * 4)
            total = ((totals[0] + totals[1]) + (totals[2] + totals[3])).astype(BF)
            if k < 2:
                ag[k] = total
                gv[core, rounds[k][2] + tile_of(k, chip)] = total
                source = ag.at[k]
            else:
                age[...] = total
                source = age
                own_copy().start()

            def one(to_g, to_o):
                pltpu.make_async_remote_copy(
                    src_ref=source, dst_ref=place(k), send_sem=ag_send.at[k],
                    recv_sem=ag_recv.at[k], device_id=(to_g, to_o), device_id_type=MESH).start()
            others(one, cores=(0,) if k < 2 else (1, 0))

    def swap_copy(k):
        part = gv.at[core, pl.ds(rounds[k][2], rounds[k][0])]
        return pltpu.make_async_remote_copy(
            src_ref=part, dst_ref=part, send_sem=swap_send.at[k], recv_sem=swap_recv.at[k],
            device_id=(g + 1 - 2 * core, o), device_id_type=MESH)

    def swap_start(k):
        count = rounds[k][0]

        @pl.when(tile_of(k, chip) < count)
        def _():
            span_wait(gr.at[k], count - 1, ag_recv.at[k], "recv")

        @pl.when(tile_of(k, chip) >= count)
        def _():
            span_wait(gr.at[k], count, ag_recv.at[k], "recv")
        swap_copy(k).start()

    def out_copy(k):
        part = pl.ds(rounds[k][2], rounds[k][0])
        return pltpu.make_async_copy(gv.at[:, part], gall.at[:, part], own_sem.at[k])

    def out_start(k):
        swap_copy(k).wait_recv()
        out_copy(k).start()

    def finish_enc():
        count = rounds[2][0]
        pair_copy(2).wait_send()

        @pl.when(tile_of(2, chip) < count)
        def _():
            own_copy().wait()
            span_wait(gre, count - 1, rs_send.at[2], "send")
            span_wait(gre, n_dev - 1, ag_send.at[2], "send")
            span_wait(gre, 2 * count - 1, ag_recv.at[2], "recv")

        @pl.when(tile_of(2, chip) >= count)
        def _():
            span_wait(gre, count, rs_send.at[2], "send")
            span_wait(gre, 2 * count, ag_recv.at[2], "recv")

    def finish(k):
        count = rounds[k][0]
        pair_copy(k).wait_send()
        swap_copy(k).wait_send()

        @pl.when(tile_of(k, chip) < count)
        def _():
            span_wait(gr.at[k], count - 1, rs_send.at[k], "send")
            span_wait(gr.at[k], n_chip - 1, ag_send.at[k], "send")

        @pl.when(tile_of(k, chip) >= count)
        def _():
            span_wait(gr.at[k], count, rs_send.at[k], "send")
        out_copy(k).wait()

    back_rims(1)
    back_own(1)
    layer_weights(1, act1, gm1, g1)
    pair_copy(0).start()
    loop(n_edge // CH, slopes)
    scatter_start(0)
    loop(n_edge // CH, last_messages)
    gather_messages(1)
    add_rims(1)

    def back_first(c):
        at = chunk(c)
        rows = (mm(dd[at, :], gh[...].astype(BF)) * wide(ecol[at, :])).astype(BF)
        gm0[at, :] = rows
        gp[at, :] = (mt(rows, msg_proj[0]) * pre0[at, :]).astype(BF)

    loop(n_edge // CH, back_first)
    back_rims(0)
    gather_start(0)
    back_own(0)
    layer_weights(0, act0, gm0, g0)
    pair_copy(1).start()
    scatter_start(1)
    add_rims(0)

    acc[...] = jnp.zeros_like(acc)

    def encode_out(c):
        at = chunk(c)
        rows = (mm(pp[at, :], gh[...].astype(BF)) * wide(ccol[at, :])).astype(BF)
        acc[...] += tm(eact[at, :], rows)
        cemb[at, :] = (mt(rows, enc_out[...]) * edsilu[at, :]).astype(BF)

    loop(n_col // CH, encode_out)
    halves(ge, 0, acc[...])
    acc[...] = jnp.zeros_like(acc)

    def encode_in(c):
        at = chunk(c)
        acc[0:128, :] += tm(rx[at, :], cemb[at, :])

    loop(n_col // CH, encode_in)
    halves(ge, 256, acc[0:128, :])
    pair_copy(2).start()
    scatter_start(2)
    gather_start(1)
    swap_start(0)
    out_start(0)
    gather_start(2)
    swap_start(1)
    out_start(1)

    cols_done.wait_send()
    aux_done.wait_send()
    for l in range(2):
        for r in range(4):
            @pl.when(here[flip[r]])
            def _():
                fwd_copy(l, r).wait_send()

            @pl.when(here[r])
            def _():
                back_copy(l, r).wait_send()
    for k in range(2):
        finish(k)
    finish_enc()


def finish_kernel(gall, gall_enc, node_in, enc_in_g, enc_out_g, src_g, dst_g, msg_g, node_out,
                  tiles, tiles_enc, mats, nodes, in_sem, out_sem):
    jobs = []
    for layer, first in ((1, 0), (0, 48)):
        for m, ref in enumerate((src_g, dst_g, msg_g)):
            jobs.append((gall, tiles, first + 16 * m, 16, ref.at[layer]))
    jobs.append((gall_enc, tiles_enc, 0, 32, enc_out_g))
    jobs.append((gall_enc, tiles_enc, 32, 16, enc_in_g))
    n = len(jobs)

    def fetch(i):
        source, held, first, count, _ = jobs[i]
        at = pl.ds(first, count)
        return pltpu.make_async_copy(source.at[:, at], held.at[:, at], in_sem.at[i])

    def put(i):
        target = jobs[i][4]
        return pltpu.make_async_copy(mats.at[i, pl.ds(0, target.shape[0])], target, out_sem.at[i])

    node_fetch = pltpu.make_async_copy(node_in, nodes, in_sem.at[n])
    node_put = pltpu.make_async_copy(nodes, node_out, out_sem.at[n])
    for i in range(n):
        fetch(i).start()
    node_fetch.start()
    for i in range(n):
        fetch(i).wait()
        _, held, first, count, target = jobs[i]
        n_row = target.shape[0]
        for half in range(2):
            block = held[half, first:first + count].astype(F32).reshape(n_row, LANES)
            mats[i, 0:n_row, half * LANES:(half + 1) * LANES] = block
        put(i).start()
    node_fetch.wait()
    node_put.start()
    for i in range(n):
        put(i).wait()
    node_put.wait()


def per_device(n_grid, n_dom, columns, column_live, col_weight, col_slot, node_static, boundary_idx,
               edge_src, edge_dst, edge_live, edge_weight, enc_in, enc_out, src_proj, dst_proj, msg_proj,
               node_cotangent):
    n_dev = n_grid * n_dom
    n_col = columns.shape[0]
    n_edge = edge_src.shape[0]
    n_node, width = node_static.shape
    n_bnd = boundary_idx.shape[0]
    rows = lambda x: x.reshape(-1, LANES)
    vm = lambda *shape: pltpu.VMEM(shape, BF)
    vf = lambda *shape: pltpu.VMEM(shape, F32)
    dma = pltpu.SemaphoreType.DMA
    args = (columns, rows(column_live), rows(col_weight), rows(col_slot), node_static, rows(boundary_idx),
            rows(edge_src), rows(edge_dst), rows(edge_live), rows(edge_weight), enc_in, enc_out, src_proj,
            dst_proj, msg_proj, node_cotangent)
    scratch = [pltpu.VMEM(a.shape, a.dtype) for a in args] + [
        dma((len(args),)), pltpu.SemaphoreType.REGULAR,
        vf(n_dev, LANES), vf(n_dev, LANES), vm(n_col, columns.shape[1]), vf(n_col // LANES, LANES),
        vf(n_col // LANES, LANES), vf(n_col, LANES), vf(n_edge, LANES),
        vm(n_edge, n_node), vm(n_edge, 4 * n_bnd), vm(n_node, n_edge), vm(4 * n_bnd, n_edge),
        vm(n_edge, n_node), vm(n_node, n_edge), vm(n_bnd, n_node), vm(n_node, n_bnd),
        vm(n_col, n_node), vm(n_node, n_col),
        vm(2, n_node, width), vm(2, 4, n_bnd, width), vm(2, n_bnd, width), vm(2, 4, n_bnd, width),
        vm(2, 4, n_bnd, width),
        vm(n_col, width), vf(n_col, width), vm(n_col, width), vf(n_edge, width), vf(n_edge, width),
        vm(n_edge, width), vm(n_edge, width), vm(n_edge, width), vm(n_edge, width), vm(n_edge, width),
        vf(n_edge, width), vm(n_edge, width), vm(n_node, width), vm(4, n_bnd, width), vm(n_node, width),
        vf(n_node, width),
        vf(width, width), vf(2, 768, LANES), vf(2, 768, LANES), vf(2, 384, LANES),
        vf(768, LANES), vf(768, LANES), vf(384, LANES), vm(768, LANES), vm(768, LANES), vm(48, 8, LANES),
        vm(2, n_dev // 2, TILE, LANES), vm(n_dev, 8, LANES), vm(2, TILE, LANES), vm(8, LANES),
        vm(2, 96, TILE, LANES),
        pltpu.VMEM((n_bnd, LANES), jnp.int32), vm(n_bnd, n_edge), vm(n_bnd, n_col), vm(n_edge, width),
        dma((3,)), dma((3,)), dma((3,)), dma((3,)),
        dma(()), dma((n_grid // 2,)), dma(()), dma(()), dma((2, 4)), dma((2, 4)), dma((2, 4)), dma((2, 4)),
        dma((3,)), dma((3,)), dma((3,)), dma((3,)), dma((3,)),
    ]
    in_vmem = pl.BlockSpec(memory_space=pltpu.VMEM)
    in_hbm = pl.BlockSpec(memory_space=pl.ANY)
    node_out, gall, gall_enc = pl.pallas_call(
        functools.partial(step_kernel, n_grid, n_dom, len(args)),
        out_shape=(jax.ShapeDtypeStruct((n_node, width), BF), jax.ShapeDtypeStruct((2, 96, TILE, LANES), BF),
                   jax.ShapeDtypeStruct((2, 48, 8, LANES), BF)),
        in_specs=[pl.BlockSpec(memory_space=pl.ANY)] * len(args),
        out_specs=(in_vmem, in_hbm, in_hbm),
        scratch_shapes=scratch,
        compiler_params=pltpu.CompilerParams(
            collective_id=0, has_side_effects=True, vmem_limit_bytes=62 * 1024 * 1024),
    )(*args)
    mat = jax.ShapeDtypeStruct((width, width), F32)
    pair = jax.ShapeDtypeStruct((2, width, width), F32)
    enc_in_g, enc_out_g, src_g, dst_g, msg_g, node_final = pl.pallas_call(
        finish_kernel,
        out_shape=(jax.ShapeDtypeStruct(enc_in.shape, F32), mat, pair, pair, pair,
                   jax.ShapeDtypeStruct((n_node, width), BF)),
        in_specs=[in_hbm] * 3,
        out_specs=(in_hbm,) * 6,
        scratch_shapes=[vm(2, 96, TILE, LANES), vm(2, 48, 8, LANES), vf(8, width, width), vm(n_node, width), dma((9,)), dma((9,))],
    )(gall, gall_enc, node_out)
    return (node_final, enc_in_g, enc_out_g, src_g, dst_g, msg_g)


def solution(mesh):
    n_grid, n_dom = mesh.shape["grid"], mesh.shape["dom"]
    both = P(("grid", "dom"))
    rows = P(("grid", "dom"), None)
    placed = (rows, both, both, both, rows, both, both, both, both, both, P(), P(), P(), P(), P(), rows)
    return jax.shard_map(
        functools.partial(per_device, n_grid, n_dom),
        mesh=mesh,
        in_specs=placed,
        out_specs=(rows, P(), P(), P(), P(), P()),
        check_vma=False,
    )
```

```python
import functools

import jax
import jax.numpy as jnp
from jax import lax
from jax.experimental import pallas as pl
from jax.experimental.pallas import tpu as pltpu
from jax.sharding import PartitionSpec as P

MESH = pl.DeviceIdType.MESH
BF = jnp.bfloat16
F32 = jnp.float32
CH = 1024
CN = 512
LANES = 128
TILE = 16


def mm(a, b):
    return lax.dot_general(a, b, (((1,), (0,)), ((), ())), preferred_element_type=F32)


def mt(a, b):
    return lax.dot_general(a, b, (((1,), (1,)), ((), ())), preferred_element_type=F32)


def tm(a, b):
    return lax.dot_general(a, b, (((0,), (0,)), ((), ())), preferred_element_type=F32)


def wide(x):
    return jnp.concatenate([x, x], axis=1)


def hot(equal):
    return jnp.where(equal, 1.0, 0.0).astype(BF)


def step_kernel(
    n_grid, n_dom,
    n_in, *refs,
):
    inputs = refs[:n_in]
    outs = refs[n_in:n_in + 3]
    copies = refs[n_in + 3:2 * n_in + 3]
    step_body(n_grid, n_dom, inputs, copies, *outs, *refs[2 * n_in + 3:])


def step_body(
    n_grid, n_dom, inputs, copies, node_out, gall, gall_enc,
    in_sem, round_sem, aux_tx, aux_rx, rx, srow, crow, ccol, ecol,
    so, sr, sot, srt, dd, ddt, bb, bbt, pp, ppt,
    hh, rim, rim_tx, gt_tx, gt_rx,
    eact, edsilu, cemb, pre0, pre1, act0, act1, msg, gm0, gm1, ga1, gp, gs_own, gs_rim, gd, gh,
    acc, g1, g0, ge, px1, px0, pxe, tx1, tx0, txe, gr, gre, ag, age, gv, bcol, bdt, bpt, xs, swap_send, swap_recv,
    pair_send, pair_recv,
    a2a_send, a2a_recv, aux_send, aux_recv, rim_send, rim_recv, gt_send, gt_recv,
    rs_send, rs_recv, ag_send, ag_recv, own_sem,
):
    (cols, live, cweight, slot, static, bidx, esrc, edst, elive, eweight,
     enc_in, enc_out, src_proj, dst_proj, msg_proj, cot) = copies
    n_dev = n_grid * n_dom
    n_node = static.shape[0]
    n_edge = so.shape[0]
    n_col = cols.shape[0]
    n_bnd = bb.shape[0]
    rows_e = n_edge // LANES
    rows_c = n_col // LANES
    g = lax.axis_index("grid")
    o = lax.axis_index("dom")
    me = g * n_dom + o

    core = lax.rem(g, 2)
    z = g // 2
    n_z, n_y, n_x = n_grid // 2, n_dom // 4, 4
    y, x = o // n_x, lax.rem(o, n_x)
    chip = z * n_dom + o
    n_chip = n_dev // 2

    def others(fn, cores=(1, 0)):
        def some(i, skip):
            to_z = lax.rem(z + (n_z - 1 - i // n_y), n_z)
            to_y = lax.rem(y + (n_y - 1 - lax.rem(i, n_y)), n_y)
            for dx in (2, 1, 3, 0):
                to_o = to_y * n_x + lax.rem(x + dx, n_x)
                for dc in cores:
                    if not (skip and dx == 0 and dc == 0):
                        fn(to_z * 2 + (1 - core if dc else core), to_o)

        def body(i, carry):
            some(i, False)
            return carry
        lax.fori_loop(0, n_z * n_y - 1, body, 0)
        some(n_z * n_y - 1, True)

    def loop(n, fn):
        def body(k, carry):
            fn(k)
            return carry
        lax.fori_loop(0, n, body, 0)

    def load(i):
        return pltpu.make_async_copy(inputs[i], copies[i], in_sem.at[i])

    barrier = pltpu.get_barrier_semaphore()

    def column(fn):
        for k in range(1, n_grid):
            fn((lax.rem(g + k, n_grid), o))

    def greet(sem, to):
        pl.semaphore_signal(sem, inc=1, device_id=to, device_id_type=MESH)

    for k in range(1, n_dom):
        greet(barrier, (g, lax.rem(o + k, n_dom)))
    column(lambda to: greet(barrier, to))
    order = (0, 1, 2, 3, 6, 7, 8, 9, 5, 15, 14, 10, 11, 4, 12, 13)
    for i in order:
        load(i).start()
    for i in order[:4]:
        load(i).wait()

    lane = lax.broadcasted_iota(jnp.int32, (rows_c, LANES), 1)
    quarter = lax.rem(me, 4)
    slot_f = slot[...].astype(F32)
    scale_f = cweight[...] * live[...].astype(F32)
    for j in range(8):
        to_slot = lax.rem((quarter - j) * 16 + 2 * LANES, LANES)
        to_scale = lax.rem((quarter - j) * 16 + 64 + 2 * LANES, LANES)
        a = pltpu.roll(slot_f, to_slot, axis=1)
        b = pltpu.roll(scale_f, to_scale, axis=1)
        row = jnp.where(lane // 16 == quarter, a, jnp.where(lane // 16 == quarter + 4, b, 0.0))
        aux_tx[pl.ds(j, rows_c, stride=8), :] = row

    pl.semaphore_wait(barrier, n_dom + n_grid - 2)
    column(lambda to: greet(round_sem, to))
    pl.semaphore_wait(round_sem, n_grid - 1)

    def send_aux(to_g, to_o):
        d = to_g * n_dom + to_o
        pltpu.make_async_remote_copy(
            src_ref=aux_tx.at[d], dst_ref=aux_rx.at[me],
            send_sem=aux_send, recv_sem=aux_recv, device_id=(to_g, to_o), device_id_type=MESH,
        ).start()

    def send_cols(to_g, to_o):
        d = to_g * n_dom + to_o
        pltpu.make_async_remote_copy(
            src_ref=cols.at[pl.ds(pl.multiple_of(d * TILE, TILE), TILE), :],
            dst_ref=rx.at[pl.ds(pl.multiple_of(me * TILE, TILE), TILE), :],
            send_sem=a2a_send, recv_sem=a2a_recv.at[z], device_id=(to_g, to_o), device_id_type=MESH,
        ).start()

    others(send_aux)
    others(send_cols)
    for i in order[4:]:
        load(i).wait()
    mine = pl.ds(pl.multiple_of(me * TILE, TILE), TILE)
    rx[mine, :] = cols[mine, :]
    aux_rx[me] = aux_tx[me]

    here = (g > 0, g < n_grid - 1, o > 0, o < n_dom - 1)
    near = ((g - 1, o), (g + 1, o), (g, o - 1), (g, o + 1))
    flip = (1, 0, 3, 2)
    for r in range(4):
        @pl.when(jnp.logical_not(here[r]))
        def _():
            for l in range(2):
                rim[l, r] = jnp.zeros((n_bnd, 256), BF)
                gt_rx[l, flip[r]] = jnp.zeros((n_bnd, 256), BF)

    lane_i = lax.broadcasted_iota(jnp.int32, (LANES, LANES), 1)
    sub_i = lax.broadcasted_iota(jnp.int32, (LANES, LANES), 0)

    def across(row):
        full = jnp.broadcast_to(row, (LANES, LANES))
        return full, jnp.transpose(full)

    def build_edges(b):
        at = pl.ds(pl.multiple_of(b * LANES, LANES), LANES)
        full, down = across(edst[pl.ds(b, 1), :])
        for c in range(n_node // LANES):
            part = slice(c * LANES, (c + 1) * LANES)
            dd[at, part] = hot(down == lane_i + c * LANES)
            ddt[part, at] = hot(full == sub_i + c * LANES)
        for c in range(n_bnd // LANES):
            part = slice(c * LANES, (c + 1) * LANES)
            bdt[part, at] = hot(full == bcol[part, :])
        scale = eweight[pl.ds(b, 1), :] * elive[pl.ds(b, 1), :].astype(F32)
        ecol[at, :] = across(scale)[1]
        full, down = across(esrc[pl.ds(b, 1), :])
        for c in range(n_node // LANES):
            part = slice(c * LANES, (c + 1) * LANES)
            so[at, part] = hot(down == lane_i + c * LANES)
            sot[part, at] = hot(full == sub_i + c * LANES)
        for c in range(4 * n_bnd // LANES):
            part = slice(c * LANES, (c + 1) * LANES)
            sr[at, part] = hot(down == lane_i + (n_node + c * LANES))
            srt[part, at] = hot(full == sub_i + (n_node + c * LANES))

    def build_bound(b):
        at = pl.ds(pl.multiple_of(b * LANES, LANES), LANES)
        full, down = across(bidx[pl.ds(b, 1), :])
        for c in range(n_node // LANES):
            part = slice(c * LANES, (c + 1) * LANES)
            bb[at, part] = hot(down == lane_i + c * LANES)
            bbt[part, at] = hot(full == sub_i + c * LANES)
        bcol[at, :] = down

    loop(n_bnd // LANES, build_bound)
    loop(rows_e, build_edges)

    def chunk(c):
        return pl.ds(pl.multiple_of(c * CH, CH), CH)

    def node_chunk(c):
        return pl.ds(pl.multiple_of(c * CN, CN), CN)

    def back_last(c):
        at = chunk(c)
        rows = (mm(dd[at, :], cot[...]) * wide(ecol[at, :])).astype(BF)
        gm1[at, :] = rows
        ga1[at, :] = mt(rows, msg_proj[1])

    loop(n_edge // CH, back_last)

    got = pl.ds(0, (n_dev - 1) * TILE)
    cols_done = pltpu.make_async_remote_copy(
        src_ref=rx.at[got, :], dst_ref=rx.at[got, :], send_sem=a2a_send, recv_sem=a2a_recv.at[0],
        device_id=(g, o), device_id_type=MESH)
    got_aux = pl.ds(0, n_dev - 1)
    aux_done = pltpu.make_async_remote_copy(
        src_ref=aux_rx.at[got_aux], dst_ref=aux_rx.at[got_aux], send_sem=aux_send, recv_sem=aux_recv,
        device_id=(g, o), device_id_type=MESH)
    aux_done.wait_recv()
    parts = aux_rx[...].reshape(rows_c, 8, LANES)
    low = jnp.sum(parts[:, 0:4, :], axis=1)
    high = jnp.sum(parts[:, 4:8, :], axis=1)
    srow[...] = jnp.where(lane < 64, low, pltpu.roll(high, 64, axis=1))
    crow[...] = jnp.where(lane < 64, pltpu.roll(low, 64, axis=1), high)

    lane_f = lane_i.astype(F32)
    sub_f = sub_i.astype(F32)

    def build_pool(b):
        at = pl.ds(pl.multiple_of(b * LANES, LANES), LANES)
        full, down = across(srow[pl.ds(b, 1), :])
        for c in range(n_node // LANES):
            part = slice(c * LANES, (c + 1) * LANES)
            pp[at, part] = hot(down == lane_f + float(c * LANES))
            ppt[part, at] = hot(full == sub_f + float(c * LANES))
        for c in range(n_bnd // LANES):
            part = slice(c * LANES, (c + 1) * LANES)
            bpt[part, at] = hot(full == bcol[part, :].astype(F32))
        ccol[at, :] = across(crow[pl.ds(b, 1), :])[1]

    loop(rows_c, build_pool)

    def sigmoid(v):
        return 0.5 * jnp.tanh(0.5 * v) + 0.5

    plane = n_col // n_z

    def encode(to_z):
        at = pl.ds(pl.multiple_of(to_z * plane, plane), plane)
        v = mm(rx[at, :], enc_in[...])
        s = sigmoid(v)
        a = (v * s).astype(BF)
        eact[at, :] = a
        edsilu[at, :] = s * (1.0 + v * (1.0 - s))
        cemb[at, :] = (mm(a, enc_out[...]) * wide(ccol[at, :])).astype(BF)

    for dz in reversed(range(n_z)):
        from_z = lax.rem(z - dz + n_z, n_z)
        got = pl.ds(0, plane - (TILE if dz == 0 else 0))
        pltpu.make_async_remote_copy(
            src_ref=rx.at[got, :], dst_ref=rx.at[got, :], send_sem=a2a_send, recv_sem=a2a_recv.at[from_z],
            device_id=(g, o), device_id_type=MESH).wait_recv()
        encode(from_z)

    def pool(c):
        at = node_chunk(c)
        hh[0, at, :] = (static[at, :].astype(F32) + mm(ppt[at, :], cemb[...])).astype(BF)


    def fwd_copy(l, r):
        return pltpu.make_async_remote_copy(
            src_ref=rim_tx.at[l], dst_ref=rim.at[l, r], send_sem=rim_send.at[l, r],
            recv_sem=rim_recv.at[l, r], device_id=near[flip[r]], device_id_type=MESH)

    def back_copy(l, r):
        return pltpu.make_async_remote_copy(
            src_ref=gt_tx.at[l, r], dst_ref=gt_rx.at[l, r], send_sem=gt_send.at[l, r],
            recv_sem=gt_recv.at[l, r], device_id=near[r], device_id_type=MESH)

    def send_rims(l):
        if l == 0:
            rows = mm(bb[...], static[...]) + mm(bpt[...], cemb[...])
        else:
            rows = mm(bb[...], hh[0]) + mm(bdt[...], msg[...])
        rim_tx[l] = rows.astype(BF)
        for r in (2, 3, 0, 1):
            @pl.when(here[flip[r]])
            def _():
                fwd_copy(l, r).start()

    def wait_rims(l, blocks):
        for r in blocks:
            @pl.when(here[r])
            def _():
                fwd_copy(l, r).wait_recv()

    def layer_own(l, pre):
        def body(c):
            at = chunk(c)
            h = hh[l]
            xo = mm(so[at, :], h).astype(BF)
            xd = mm(dd[at, :], h).astype(BF)
            pre[at, :] = mm(xo, src_proj[l]) + mm(xd, dst_proj[l])
        loop(n_edge // CH, body)

    def layer_grid(l):
        def body(c):
            at = chunk(c)
            xs[at, :] = mm(sr[at, 0:2 * n_bnd], rim[l, 0:2].reshape(2 * n_bnd, 256)).astype(BF)
        loop(n_edge // CH, body)

    def layer_rest(l, pre, act):
        def body(c):
            at = chunk(c)
            xr = mm(sr[at, 2 * n_bnd:], rim[l, 2:4].reshape(2 * n_bnd, 256))
            xr = (xr + xs[at, :].astype(F32)).astype(BF)
            v = pre[at, :] + mm(xr, src_proj[l])
            s = sigmoid(v)
            a = (v * s).astype(BF)
            act[at, :] = a
            if l == 0:
                pre[at, :] = v
                msg[at, :] = (mm(a, msg_proj[l]) * wide(ecol[at, :])).astype(BF)
            else:
                gp[at, :] = (ga1[at, :] * (s * (1.0 + v * (1.0 - s)))).astype(BF)
        loop(n_edge // CH, body)

    def slopes(c):
        at = chunk(c)
        v = pre0[at, :]
        s = sigmoid(v)
        pre0[at, :] = s * (1.0 + v * (1.0 - s))

    def last_messages(c):
        at = chunk(c)
        msg[at, :] = (mm(act1[at, :], msg_proj[1]) * wide(ecol[at, :])).astype(BF)

    def gather_messages(l):
        def body(c):
            at = node_chunk(c)
            rows = (hh[l, at, :].astype(F32) + mm(ddt[at, :], msg[...])).astype(BF)
            if l == 0:
                hh[1, at, :] = rows
            else:
                node_out[at, :] = rows
        loop(n_node // CN, body)

    send_rims(0)
    loop(n_node // CN, pool)
    layer_own(0, pre0)
    wait_rims(0, (0, 1))
    layer_grid(0)
    wait_rims(0, (2, 3))
    layer_rest(0, pre0, act0)
    send_rims(1)
    gather_messages(0)
    layer_own(1, pre1)
    wait_rims(1, (0, 1))
    layer_grid(1)
    wait_rims(1, (2, 3))
    layer_rest(1, pre1, act1)

    def back_rims(l):
        for r in (2, 3, 0, 1):
            rows = mm(srt[r * n_bnd:(r + 1) * n_bnd, :], gp[...]).astype(BF)
            gs_rim[r] = rows
            gt_tx[l, r] = mt(rows, src_proj[l]).astype(BF)

            @pl.when(here[r])
            def _():
                back_copy(l, r).start()

    def back_own(l):
        def body(c):
            at = node_chunk(c)
            s_rows = mm(sot[at, :], gp[...]).astype(BF)
            d_rows = mm(ddt[at, :], gp[...]).astype(BF)
            gs_own[at, :] = s_rows
            gd[at, :] = d_rows
            before = cot[at, :].astype(F32) if l == 1 else gh[at, :]
            gh[at, :] = before + mt(s_rows, src_proj[l]) + mt(d_rows, dst_proj[l])
        loop(n_node // CN, body)

    def halves(out, first, value):
        rows = slice(first, first + value.shape[0])
        out[0, rows, :] = value[:, 0:LANES]
        out[1, rows, :] = value[:, LANES:]

    def layer_weights(l, act, gm, out):
        total = tm(hh[l], gs_own[...])
        for r in range(4):
            total = total + tm(rim[l, r], gs_rim[r])
        halves(out, 0, total)
        halves(out, 256, tm(hh[l], gd[...]))
        acc[...] = jnp.zeros_like(acc)

        def body(c):
            at = chunk(c)
            acc[...] += tm(act[at, :], gm[at, :])
        loop(n_edge // CH, body)
        halves(out, 512, acc[...])

    def add_rims(l):
        for r in range(4):
            @pl.when(here[flip[r]])
            def _():
                back_copy(l, r).wait_recv()

        def body(c):
            at = node_chunk(c)
            total = gh[at, :]
            for r in range(4):
                total = total + mm(bbt[at, :], gt_rx[l, r])
            gh[at, :] = total
        loop(n_node // CN, body)

    rounds = ((48, 0, 0), (48, 48, 48), (48, 16, 0))
    parts_of = ((g1, px1, tx1), (g0, px0, tx0), (ge, pxe, txe))

    def tile_of(k, q):
        return lax.rem(q - rounds[k][1] + n_chip, n_chip)

    def pair_copy(k):
        mine, theirs, _ = parts_of[k]
        return pltpu.make_async_remote_copy(
            src_ref=mine.at[1 - core], dst_ref=theirs, send_sem=pair_send.at[k],
            recv_sem=pair_recv.at[k], device_id=(g + 1 - 2 * core, o), device_id_type=MESH)

    def rows_of(t):
        return pl.ds(pl.multiple_of(t * TILE, TILE), TILE)

    def held(k):
        return gre if k == 2 else gr.at[k]

    def scatter_start(k):
        def tile(ref, t):
            return ref.at[t] if k == 2 else ref.at[rows_of(t), :]

        count = rounds[k][0]
        mine, theirs, out = parts_of[k]
        pair_copy(k).wait_recv()

        def add(c):
            at = pl.ds(pl.multiple_of(c * LANES, LANES), LANES)
            total = mine[core, at, :] + theirs[at, :]
            if k < 2:
                out[at, :] = total.astype(BF)
            else:
                out[pl.ds(c * 16, 16)] = total.reshape(16, 8, LANES).astype(BF)
        loop(theirs.shape[0] // LANES, add)

        def one(to_g, to_o):
            t = tile_of(k, (to_g // 2) * n_dom + to_o)

            @pl.when(t < count)
            def _():
                pltpu.make_async_remote_copy(
                    src_ref=tile(out, t), dst_ref=held(k).at[chip], send_sem=rs_send.at[k],
                    recv_sem=rs_recv.at[k], device_id=(to_g, to_o), device_id_type=MESH).start()
        others(one, cores=(0,))

        @pl.when(tile_of(k, chip) < count)
        def _():
            held(k)[chip] = tile(out, tile_of(k, chip))[...]

    def span_wait(ref, n, sem, what):
        at = pl.ds(0, n)
        copy = pltpu.make_async_remote_copy(
            src_ref=ref.at[at], dst_ref=ref.at[at], send_sem=sem, recv_sem=sem,
            device_id=(g, o), device_id_type=MESH)
        if what == "recv":
            copy.wait_recv()
        else:
            copy.wait_send()

    def place(k):
        if k == 2:
            return gall_enc.at[core, tile_of(k, chip)]
        return gv.at[core, rounds[k][2] + tile_of(k, chip)]

    def own_copy():
        return pltpu.make_async_copy(age, place(2), own_sem.at[2])

    def gather_start(k):
        @pl.when(tile_of(k, chip) < rounds[k][0])
        def _():
            span_wait(held(k), n_chip - 1, rs_recv.at[k], "recv")

            def body(s, totals):
                return tuple(
                    totals[i] + held(k)[s * 8 + i].astype(F32) + held(k)[s * 8 + i + 4].astype(F32)
                    for i in range(4))
            zero = jnp.zeros((8 if k == 2 else TILE, LANES), F32)
            totals = lax.fori_loop(0, n_chip // 8, body, (zero,) * 4)
            total = ((totals[0] + totals[1]) + (totals[2] + totals[3])).astype(BF)
            if k < 2:
                ag[k] = total
                gv[core, rounds[k][2] + tile_of(k, chip)] = total
                source = ag.at[k]
            else:
                age[...] = total
                source = age
                own_copy().start()

            def one(to_g, to_o):
                pltpu.make_async_remote_copy(
                    src_ref=source, dst_ref=place(k), send_sem=ag_send.at[k],
                    recv_sem=ag_recv.at[k], device_id=(to_g, to_o), device_id_type=MESH).start()
            others(one, cores=(0,) if k < 2 else (1, 0))

    def swap_copy(k):
        part = gv.at[core, pl.ds(rounds[k][2], rounds[k][0])]
        return pltpu.make_async_remote_copy(
            src_ref=part, dst_ref=part, send_sem=swap_send.at[k], recv_sem=swap_recv.at[k],
            device_id=(g + 1 - 2 * core, o), device_id_type=MESH)

    def swap_start(k):
        count = rounds[k][0]

        @pl.when(tile_of(k, chip) < count)
        def _():
            span_wait(gr.at[k], count - 1, ag_recv.at[k], "recv")

        @pl.when(tile_of(k, chip) >= count)
        def _():
            span_wait(gr.at[k], count, ag_recv.at[k], "recv")
        swap_copy(k).start()

    def out_copy(k):
        part = pl.ds(rounds[k][2], rounds[k][0])
        return pltpu.make_async_copy(gv.at[:, part], gall.at[:, part], own_sem.at[k])

    def out_start(k):
        swap_copy(k).wait_recv()
        out_copy(k).start()

    def finish_enc():
        count = rounds[2][0]
        pair_copy(2).wait_send()

        @pl.when(tile_of(2, chip) < count)
        def _():
            own_copy().wait()
            span_wait(gre, count - 1, rs_send.at[2], "send")
            span_wait(gre, n_dev - 1, ag_send.at[2], "send")
            span_wait(gre, 2 * count - 1, ag_recv.at[2], "recv")

        @pl.when(tile_of(2, chip) >= count)
        def _():
            span_wait(gre, count, rs_send.at[2], "send")
            span_wait(gre, 2 * count, ag_recv.at[2], "recv")

    def finish(k):
        count = rounds[k][0]
        pair_copy(k).wait_send()
        swap_copy(k).wait_send()

        @pl.when(tile_of(k, chip) < count)
        def _():
            span_wait(gr.at[k], count - 1, rs_send.at[k], "send")
            span_wait(gr.at[k], n_chip - 1, ag_send.at[k], "send")

        @pl.when(tile_of(k, chip) >= count)
        def _():
            span_wait(gr.at[k], count, rs_send.at[k], "send")
        out_copy(k).wait()

    back_rims(1)
    back_own(1)
    layer_weights(1, act1, gm1, g1)
    pair_copy(0).start()
    loop(n_edge // CH, slopes)
    scatter_start(0)
    loop(n_edge // CH, last_messages)
    gather_messages(1)
    add_rims(1)

    def back_first(c):
        at = chunk(c)
        rows = (mm(dd[at, :], gh[...].astype(BF)) * wide(ecol[at, :])).astype(BF)
        gm0[at, :] = rows
        gp[at, :] = (mt(rows, msg_proj[0]) * pre0[at, :]).astype(BF)

    loop(n_edge // CH, back_first)
    back_rims(0)
    back_own(0)
    layer_weights(0, act0, gm0, g0)
    pair_copy(1).start()
    gather_start(0)
    scatter_start(1)
    add_rims(0)

    acc[...] = jnp.zeros_like(acc)

    def encode_out(c):
        at = chunk(c)
        rows = (mm(pp[at, :], gh[...].astype(BF)) * wide(ccol[at, :])).astype(BF)
        acc[...] += tm(eact[at, :], rows)
        cemb[at, :] = (mt(rows, enc_out[...]) * edsilu[at, :]).astype(BF)

    loop(n_col // CH, encode_out)
    halves(ge, 0, acc[...])
    acc[...] = jnp.zeros_like(acc)

    def encode_in(c):
        at = chunk(c)
        acc[0:128, :] += tm(rx[at, :], cemb[at, :])

    loop(n_col // CH, encode_in)
    halves(ge, 256, acc[0:128, :])
    pair_copy(2).start()
    scatter_start(2)
    gather_start(1)
    swap_start(0)
    out_start(0)
    gather_start(2)
    swap_start(1)
    out_start(1)

    cols_done.wait_send()
    aux_done.wait_send()
    for l in range(2):
        for r in range(4):
            @pl.when(here[flip[r]])
            def _():
                fwd_copy(l, r).wait_send()

            @pl.when(here[r])
            def _():
                back_copy(l, r).wait_send()
    for k in range(2):
        finish(k)
    finish_enc()


def finish_kernel(gall, gall_enc, node_in, enc_in_g, enc_out_g, src_g, dst_g, msg_g, node_out,
                  tiles, tiles_enc, mats, nodes, in_sem, out_sem):
    jobs = []
    for layer, first in ((1, 0), (0, 48)):
        for m, ref in enumerate((src_g, dst_g, msg_g)):
            jobs.append((gall, tiles, first + 16 * m, 16, ref.at[layer]))
    jobs.append((gall_enc, tiles_enc, 0, 32, enc_out_g))
    jobs.append((gall_enc, tiles_enc, 32, 16, enc_in_g))
    n = len(jobs)

    def fetch(i):
        source, held, first, count, _ = jobs[i]
        at = pl.ds(first, count)
        return pltpu.make_async_copy(source.at[:, at], held.at[:, at], in_sem.at[i])

    def put(i):
        target = jobs[i][4]
        return pltpu.make_async_copy(mats.at[i, pl.ds(0, target.shape[0])], target, out_sem.at[i])

    node_fetch = pltpu.make_async_copy(node_in, nodes, in_sem.at[n])
    node_put = pltpu.make_async_copy(nodes, node_out, out_sem.at[n])
    for i in range(n):
        fetch(i).start()
    node_fetch.start()
    for i in range(n):
        fetch(i).wait()
        _, held, first, count, target = jobs[i]
        n_row = target.shape[0]
        for half in range(2):
            block = held[half, first:first + count].astype(F32).reshape(n_row, LANES)
            mats[i, 0:n_row, half * LANES:(half + 1) * LANES] = block
        put(i).start()
    node_fetch.wait()
    node_put.start()
    for i in range(n):
        put(i).wait()
    node_put.wait()


def per_device(n_grid, n_dom, columns, column_live, col_weight, col_slot, node_static, boundary_idx,
               edge_src, edge_dst, edge_live, edge_weight, enc_in, enc_out, src_proj, dst_proj, msg_proj,
               node_cotangent):
    n_dev = n_grid * n_dom
    n_col = columns.shape[0]
    n_edge = edge_src.shape[0]
    n_node, width = node_static.shape
    n_bnd = boundary_idx.shape[0]
    rows = lambda x: x.reshape(-1, LANES)
    vm = lambda *shape: pltpu.VMEM(shape, BF)
    vf = lambda *shape: pltpu.VMEM(shape, F32)
    dma = pltpu.SemaphoreType.DMA
    args = (columns, rows(column_live), rows(col_weight), rows(col_slot), node_static, rows(boundary_idx),
            rows(edge_src), rows(edge_dst), rows(edge_live), rows(edge_weight), enc_in, enc_out, src_proj,
            dst_proj, msg_proj, node_cotangent)
    scratch = [pltpu.VMEM(a.shape, a.dtype) for a in args] + [
        dma((len(args),)), pltpu.SemaphoreType.REGULAR,
        vf(n_dev, LANES), vf(n_dev, LANES), vm(n_col, columns.shape[1]), vf(n_col // LANES, LANES),
        vf(n_col // LANES, LANES), vf(n_col, LANES), vf(n_edge, LANES),
        vm(n_edge, n_node), vm(n_edge, 4 * n_bnd), vm(n_node, n_edge), vm(4 * n_bnd, n_edge),
        vm(n_edge, n_node), vm(n_node, n_edge), vm(n_bnd, n_node), vm(n_node, n_bnd),
        vm(n_col, n_node), vm(n_node, n_col),
        vm(2, n_node, width), vm(2, 4, n_bnd, width), vm(2, n_bnd, width), vm(2, 4, n_bnd, width),
        vm(2, 4, n_bnd, width),
        vm(n_col, width), vf(n_col, width), vm(n_col, width), vf(n_edge, width), vf(n_edge, width),
        vm(n_edge, width), vm(n_edge, width), vm(n_edge, width), vm(n_edge, width), vm(n_edge, width),
        vf(n_edge, width), vm(n_edge, width), vm(n_node, width), vm(4, n_bnd, width), vm(n_node, width),
        vf(n_node, width),
        vf(width, width), vf(2, 768, LANES), vf(2, 768, LANES), vf(2, 384, LANES),
        vf(768, LANES), vf(768, LANES), vf(384, LANES), vm(768, LANES), vm(768, LANES), vm(48, 8, LANES),
        vm(2, n_dev // 2, TILE, LANES), vm(n_dev, 8, LANES), vm(2, TILE, LANES), vm(8, LANES),
        vm(2, 96, TILE, LANES),
        pltpu.VMEM((n_bnd, LANES), jnp.int32), vm(n_bnd, n_edge), vm(n_bnd, n_col), vm(n_edge, width),
        dma((3,)), dma((3,)), dma((3,)), dma((3,)),
        dma(()), dma((n_grid // 2,)), dma(()), dma(()), dma((2, 4)), dma((2, 4)), dma((2, 4)), dma((2, 4)),
        dma((3,)), dma((3,)), dma((3,)), dma((3,)), dma((3,)),
    ]
    in_vmem = pl.BlockSpec(memory_space=pltpu.VMEM)
    in_hbm = pl.BlockSpec(memory_space=pl.ANY)
    node_out, gall, gall_enc = pl.pallas_call(
        functools.partial(step_kernel, n_grid, n_dom, len(args)),
        out_shape=(jax.ShapeDtypeStruct((n_node, width), BF), jax.ShapeDtypeStruct((2, 96, TILE, LANES), BF),
                   jax.ShapeDtypeStruct((2, 48, 8, LANES), BF)),
        in_specs=[pl.BlockSpec(memory_space=pl.ANY)] * len(args),
        out_specs=(in_vmem, in_hbm, in_hbm),
        scratch_shapes=scratch,
        compiler_params=pltpu.CompilerParams(
            collective_id=0, has_side_effects=True, vmem_limit_bytes=62 * 1024 * 1024),
    )(*args)
    mat = jax.ShapeDtypeStruct((width, width), F32)
    pair = jax.ShapeDtypeStruct((2, width, width), F32)
    enc_in_g, enc_out_g, src_g, dst_g, msg_g, node_final = pl.pallas_call(
        finish_kernel,
        out_shape=(jax.ShapeDtypeStruct(enc_in.shape, F32), mat, pair, pair, pair,
                   jax.ShapeDtypeStruct((n_node, width), BF)),
        in_specs=[in_hbm] * 3,
        out_specs=(in_hbm,) * 6,
        scratch_shapes=[vm(2, 96, TILE, LANES), vm(2, 48, 8, LANES), vf(8, width, width), vm(n_node, width), dma((9,)), dma((9,))],
    )(gall, gall_enc, node_out)
    return (node_final, enc_in_g, enc_out_g, src_g, dst_g, msg_g)


def solution(mesh):
    n_grid, n_dom = mesh.shape["grid"], mesh.shape["dom"]
    both = P(("grid", "dom"))
    rows = P(("grid", "dom"), None)
    placed = (rows, both, both, both, rows, both, both, both, both, both, P(), P(), P(), P(), P(), rows)
    return jax.shard_map(
        functools.partial(per_device, n_grid, n_dom),
        mesh=mesh,
        in_specs=placed,
        out_specs=(rows, P(), P(), P(), P(), P()),
        check_vma=False,
    )
```
